256 devices in a mesh: grp: 2 (over z_hi), gx: 16 (over y, z_lo), gy: 8 (over x, core).
Axes of the slice: x: 4, y: 4, z: 8 (z_hi: 2, z_lo: 4; z = z_hi * 4 + z_lo), core: 2. Of those that a mesh axis runs over, the one named last changes fastest.
Arguments:
- warmth_anomaly: float32 [64, 256, 1024], P('grp', 'gx', 'gy'), may hold values from -6 to 6
- humidity_anomaly: float32 [64, 256, 1024], P('grp', 'gx', 'gy'), may hold values from -6 to 6
- horizontal_line_advective_ratio: float32 [64], replicated, may hold values from -0.5 to 0.5
- vertical_line_advective_ratio: float32 [64], replicated, may hold values from -0.5 to 0.5
- molecular_extinction_coefficient: float32 [112], replicated, may hold values from 0.002 to 0.05
- droplet_extinction_thickness: float32 [112], replicated, may hold values from 0.005 to 0.1
- shortwave_quadrature_share: float32 [112], replicated, may hold values from 0.5 to 5
- longwave_quadrature_share: float32 [112], replicated, may hold values from 0.5 to 5
- overcast_layer_flags: int32 [65536, 64], P(('grp', 'gx', 'gy')), may hold values 0 or 1
- profile_position_within_tile: int32 [128, 512], P('gx', 'gy'), may hold values from 0 to 511, as said below
Outputs:
- temperature_out: float32 [64, 256, 1024], P('grp', 'gx', 'gy')
- moisture_out: float32 [64, 256, 1024], P('grp', 'gx', 'gy')
- warming_rates: float32 [65536, 64], P(('grp', 'gx', 'gy'))
The draws below stay inside these ranges and needn't reach their ends.
Inputs may be any that keep to these rules, and one draw needn't show every extreme that they name: `profile_position_within_tile`: each tile's block of 8 x 64 entries holds every number from 0 to 511 exactly once.
All inputs are finite; a program needn't handle non-finite values. No bound on the sum of `overcast_layer_flags` on one device may be relied on, other than what follows from the above.
Results may differ from the reference program's by a relative error of at most 0.000092.
Values sent between devices are 32-bit elements; how exact they have to be, the bound alone decides.
A program may use at most 64 MiB of HBM per device.

```python
import math
import jax
import jax.numpy as jnp
from jax import lax

VERTICAL_LAYERS = 64
G = 112
SWEEPS = 8
MESH_HEIGHT = 256
MESH_WIDTH = 1024
CXC = 8
CYC = 64
NXC = 128
NYC = 512
SLOTS = 512
BATCH_PROFILES = 256
NB = 65536
N_GRP = 2
N_GX = 16
N_GY = 8


def draw_profile_position_within_tile(key, part):
    tiles_x = NXC // CXC
    tiles_y = NYC // CYC
    keys = jax.random.split(key, tiles_x * tiles_y)
    perms = jax.vmap(lambda subkey: jax.random.permutation(subkey, CXC * CYC))(keys)
    perms = perms.reshape(tiles_x, tiles_y, CXC, CYC).transpose(0, 2, 1, 3)
    return perms.reshape(NXC, NYC).astype(jnp.int32)


def set_ends(values, stream_key, least, high):
    longest = values.shape.index(max(values.shape))
    spots = []
    for shift in (0, 1):
        where = [jax.random.randint(jax.random.fold_in(stream_key, axis), (), 0, length) for axis, length in enumerate(values.shape)]
        where[longest] = (where[longest] + shift) % values.shape[longest]
        spots.append(tuple(where))
    return values.at[spots[0]].set(least).at[spots[1]].set(high)


def levels(stream_key, shape, shards, least, high):
    def one(dim, shards_of):
        heights = jax.random.uniform(jax.random.fold_in(jax.random.fold_in(stream_key, 6), dim), (shards_of,), jnp.float32, least / len(shards), high / len(shards))
        return jnp.repeat(jnp.exp(heights), shape[dim] // shards_of).reshape((-1,) + (1,) * (len(shape) - dim - 1))

    gain = one(*shards[0])
    for cut in shards[1:]:
        gain = gain * one(*cut)
    return gain


def gaussian(stream_key, extent, spread, reach, cuts=(), kind=jnp.bfloat16):
    array = spread * jax.random.normal(stream_key, extent, jnp.float32)
    if cuts:
        array = array * levels(stream_key, extent, cuts, -0.22, 0.18)
    return jnp.clip(array, -reach, reach).astype(kind)


def setup_inputs(seed: int = 0) -> dict:
    splits = jax.random.split(jax.random.key(seed), 11)
    warmth_anomaly = gaussian(splits[0], (VERTICAL_LAYERS, MESH_HEIGHT, MESH_WIDTH), 1.0, 6.0, ((0, 2), (1, 16), (2, 8)), jnp.float32)
    humidity_anomaly = gaussian(splits[1], (VERTICAL_LAYERS, MESH_HEIGHT, MESH_WIDTH), 1.0, 6.0, ((0, 2), (1, 16), (2, 8)), jnp.float32)
    horizontal_line_advective_ratio = jnp.clip(jax.random.uniform(splits[2], (VERTICAL_LAYERS,), jnp.float32, -0.5, 0.5), -0.5, 0.5)
    vertical_line_advective_ratio = jnp.clip(jax.random.uniform(splits[3], (VERTICAL_LAYERS,), jnp.float32, -0.5, 0.5), -0.5, 0.5)
    molecular_extinction_coefficient = jnp.clip(jnp.exp(jax.random.uniform(splits[4], (G,), jnp.float32, math.log(0.002), math.log(0.05))), 0.002, 0.05)
    droplet_extinction_thickness = jnp.clip(jnp.exp(jax.random.uniform(splits[5], (G,), jnp.float32, math.log(0.005), math.log(0.1))), 0.005, 0.1)
    shortwave_quadrature_share = jnp.clip(jnp.exp(jax.random.uniform(splits[6], (G,), jnp.float32, math.log(0.5), math.log(5.0))), 0.5, 5.0)
    longwave_quadrature_share = jnp.clip(jnp.exp(jax.random.uniform(splits[7], (G,), jnp.float32, math.log(0.5), math.log(5.0))), 0.5, 5.0)
    overcast_layer_flags = set_ends((jax.random.randint(splits[8], (NB, VERTICAL_LAYERS), 0, 2) < 1).astype(jnp.int32), jax.random.fold_in(splits[8], 1), 0, 1)
    profile_position_within_tile = draw_profile_position_within_tile(jax.random.fold_in(splits[10], 71), 0)
    return dict(warmth_anomaly=warmth_anomaly, humidity_anomaly=humidity_anomaly, horizontal_line_advective_ratio=horizontal_line_advective_ratio, vertical_line_advective_ratio=vertical_line_advective_ratio, molecular_extinction_coefficient=molecular_extinction_coefficient, droplet_extinction_thickness=droplet_extinction_thickness, shortwave_quadrature_share=shortwave_quadrature_share, longwave_quadrature_share=longwave_quadrature_share, overcast_layer_flags=overcast_layer_flags, profile_position_within_tile=profile_position_within_tile)


NU_H = 0.15
NU_V = 0.15
HEATING_INTERVAL = 0.5


def advance_variable(grid_field, horizontal_line_advective_ratio, vertical_line_advective_ratio):
    row_next = jnp.roll(grid_field, -1, 1)
    row_prev = jnp.roll(grid_field, 1, 1)
    col_next = jnp.roll(grid_field, -1, 2)
    col_prev = jnp.roll(grid_field, 1, 2)
    padded = jnp.pad(grid_field, ((1, 1), (0, 0), (0, 0)))
    lev_next = padded[2:]
    lev_prev = padded[:-2]
    speed_x = horizontal_line_advective_ratio[:, None, None]
    speed_y = vertical_line_advective_ratio[:, None, None]
    return (grid_field - 0.5 * speed_x * (row_next - row_prev) - 0.5 * speed_y * (col_next - col_prev)
            + NU_H * (row_next + row_prev + col_next + col_prev - 4.0 * grid_field)
            + NU_V * (lev_next + lev_prev - 2.0 * grid_field))


def reduce_mesh_resolution(grid_field):
    return grid_field.reshape(VERTICAL_LAYERS, NXC, 2, NYC, 2).mean(axis=(2, 4))


def tile_slots(profile_position_within_tile):
    return profile_position_within_tile.reshape(N_GX, CXC, N_GY, CYC).transpose(0, 2, 1, 3).reshape(N_GX, N_GY, SLOTS)


def collect_profiles(coarse, profile_position_within_tile):
    tiles = coarse.reshape(VERTICAL_LAYERS, N_GX, CXC, N_GY, CYC).transpose(1, 3, 2, 4, 0).reshape(N_GX, N_GY, SLOTS, VERTICAL_LAYERS)
    inverse = jnp.argsort(tile_slots(profile_position_within_tile), axis=2).astype(jnp.int32)
    packed = jnp.take_along_axis(tiles, inverse[:, :, :, None], axis=2)
    return packed.reshape(N_GX, N_GY, N_GRP, BATCH_PROFILES, VERTICAL_LAYERS).transpose(2, 0, 1, 3, 4).reshape(NB, VERTICAL_LAYERS)


def unpack_columns(warming_rates, profile_position_within_tile):
    tiles = warming_rates.reshape(N_GRP, N_GX, N_GY, BATCH_PROFILES, VERTICAL_LAYERS).transpose(1, 2, 0, 3, 4).reshape(N_GX, N_GY, SLOTS, VERTICAL_LAYERS)
    placed = jnp.take_along_axis(tiles, tile_slots(profile_position_within_tile)[:, :, :, None], axis=2)
    return placed.reshape(N_GX, N_GY, CXC, CYC, VERTICAL_LAYERS).transpose(4, 0, 2, 1, 3).reshape(VERTICAL_LAYERS, NXC, NYC)


def refine_heat(coarse):
    even_rows = 0.75 * coarse + 0.25 * jnp.roll(coarse, 1, 1)
    odd_rows = 0.75 * coarse + 0.25 * jnp.roll(coarse, -1, 1)
    rows_done = jnp.stack([even_rows, odd_rows], axis=2).reshape(VERTICAL_LAYERS, MESH_HEIGHT, NYC)
    even_cols = 0.75 * rows_done + 0.25 * jnp.roll(rows_done, 1, 2)
    odd_cols = 0.75 * rows_done + 0.25 * jnp.roll(rows_done, -1, 2)
    return jnp.stack([even_cols, odd_cols], axis=3).reshape(VERTICAL_LAYERS, MESH_HEIGHT, MESH_WIDTH)


def radiate(theta_rows, moist_rows, mask_rows, molecular_extinction_coefficient, droplet_extinction_thickness, shortwave_quadrature_share, longwave_quadrature_share):
    absorber = jax.nn.softplus(moist_rows)
    cloudy = mask_rows.astype(jnp.float32)
    optical_depth = absorber[:, :, None] * molecular_extinction_coefficient + cloudy[:, :, None] * droplet_extinction_thickness
    optical_path_above = jnp.cumsum(optical_depth, axis=1) - optical_depth
    absorbed = 1.0 - jnp.exp(-optical_depth)
    shortwave_total = jnp.sum(shortwave_quadrature_share * jnp.exp(-optical_path_above) * absorbed, axis=2)
    longwave_total = jnp.sum(longwave_quadrature_share * absorbed, axis=2)
    return (shortwave_total - longwave_total * (1.0 + 0.1 * theta_rows)) * (4.0 / G)


def reference(warmth_anomaly, humidity_anomaly, horizontal_line_advective_ratio, vertical_line_advective_ratio, molecular_extinction_coefficient, droplet_extinction_thickness, shortwave_quadrature_share, longwave_quadrature_share, overcast_layer_flags, profile_position_within_tile):
    theta_vertical_profile = collect_profiles(reduce_mesh_resolution(warmth_anomaly), profile_position_within_tile)
    humidity_profile = collect_profiles(reduce_mesh_resolution(humidity_anomaly), profile_position_within_tile)
    partitions = NB // BATCH_PROFILES

    def within_partition(items):
        return radiate(items[0], items[1], items[2], molecular_extinction_coefficient, droplet_extinction_thickness, shortwave_quadrature_share, longwave_quadrature_share)

    warming_rates = lax.map(within_partition, (theta_vertical_profile.reshape(partitions, BATCH_PROFILES, VERTICAL_LAYERS), humidity_profile.reshape(partitions, BATCH_PROFILES, VERTICAL_LAYERS),
                                  overcast_layer_flags.reshape(partitions, BATCH_PROFILES, VERTICAL_LAYERS))).reshape(NB, VERTICAL_LAYERS)
    warming_refined = refine_heat(unpack_columns(warming_rates, profile_position_within_tile))
    present_heat_anomaly = warmth_anomaly
    humidity_present = humidity_anomaly
    for sweep_index in range(SWEEPS):
        present_heat_anomaly = advance_variable(present_heat_anomaly, horizontal_line_advective_ratio, vertical_line_advective_ratio)
        humidity_present = advance_variable(humidity_present, horizontal_line_advective_ratio, vertical_line_advective_ratio)
    return present_heat_anomaly + HEATING_INTERVAL * warming_refined, humidity_present, warming_rates
```

```python
import functools
import math

import jax
import jax.numpy as jnp
from jax import lax
from jax.experimental import pallas as pl
from jax.experimental.pallas import tpu as pltpu
from jax.sharding import PartitionSpec as P

SWEEPS = 8
NU_H = 0.15
NU_V = 0.15
HEATING_INTERVAL = 0.5
LEV = 32
ROWS = 16
COLS = 128
H = 8
PAD = 8
XL = LEV + H
XR = ROWS + 2 * H
ALL = XL + 2 * PAD
G = 112
GB = 4
F32 = jnp.float32
MESH = pl.DeviceIdType.MESH
HI = lax.Precision.HIGHEST


def lanes(shape):
    return lax.broadcasted_iota(jnp.int32, shape, len(shape) - 1)


def subs(shape):
    return lax.broadcasted_iota(jnp.int32, shape, len(shape) - 2)


def roll(x, amount, axis=1):
    n = x.shape[axis]
    amount = amount % n
    return x if amount == 0 else pltpu.roll(x, amount, axis)


def kernel(
    sizes,
    cx_ref, cy_ref, k_ref, d_ref, sw_ref, lw_ref,
    t_ref, m_ref, flags_ref, slot_ref,
    to_ref, mo_ref, wr_ref,
    fa, fb, ea, eb, coef, yst, arad, crad, trad, acc, fts, fsend, frecv, a0s, a0r, c0b,
    oh, fc, pws, wrecv, wt, cus, ews, ewl, ewr, eps, epl, epr,
    send, recv,
):
    ng, nx, ny = sizes
    g, x, y = lax.axis_index("grp"), lax.axis_index("gx"), lax.axis_index("gy")
    og = 1 - g
    xn, xp = lax.rem(x + 1, nx), lax.rem(x + nx - 1, nx)
    yn, yp = lax.rem(y + 1, ny), lax.rem(y + ny - 1, ny)
    gf = g.astype(F32)
    peers = [(og, x, y), (g, xn, y), (g, xp, y), (og, xn, y), (og, xp, y), (g, x, yn), (g, x, yp)]

    barrier = pltpu.get_barrier_semaphore()
    for peer in peers:
        pl.semaphore_signal(barrier, inc=1, device_id=peer, device_id_type=MESH)

    def copy(i, src, dst, peer):
        return pltpu.make_async_remote_copy(
            src_ref=src, dst_ref=dst, send_sem=send.at[i], recv_sem=recv.at[i],
            device_id=peer, device_id_type=MESH,
        )

    own = pl.multiple_of(PAD + H * g, 8)

    def place(r, _):
        fa[0, H + r, pl.ds(own, LEV), :] = t_ref[pl.ds(r, LEV, stride=ROWS), :]
        fa[1, H + r, pl.ds(own, LEV), :] = roll(m_ref[pl.ds(r, LEV, stride=ROWS), :], 64)
        return 0

    lax.fori_loop(0, ROWS, place, 0)
    zero8 = jnp.zeros((8, COLS), F32)

    def clear(r, _):
        for buf in (fa, fb):
            for f in range(2):
                buf[f, r, 0:PAD, :] = zero8
                buf[f, r, PAD + XL:ALL, :] = zero8
        for buf in (ea, eb):
            buf[r, 0:PAD, :] = zero8
            buf[r, PAD + XL:ALL, :] = zero8
        return 0

    lax.fori_loop(0, XR, clear, 0)

    def coefs(i, _):
        level = i + 24 * g
        hx, hy = 0.5 * cx_ref[level], 0.5 * cy_ref[level]
        for n, value in enumerate((NU_H - hx, NU_H + hx, NU_H - hy, NU_H + hy)):
            coef[n, pl.ds(i, 1), :] = jnp.full((1, COLS), value, F32)
        return 0

    lax.fori_loop(0, XL, coefs, 0)

    kk = lax.broadcasted_iota(jnp.int32, (2 * COLS, COLS), 0)
    nn = lax.broadcasted_iota(jnp.int32, (2 * COLS, COLS), 1)
    means = []
    for f in range(2):
        shift = 64 * f
        column = (kk + COLS - shift) % COLS
        pick = jnp.where(nn == (kk // COLS) * 64 + column // 2, 0.25, 0.0).astype(F32)
        parts = []
        for q in range(4):
            base = H + 4 * q
            rows = [fa[f, base + n, pl.ds(own, LEV), :] for n in range(4)]
            parts.append(jnp.concatenate([rows[0] + rows[1], rows[2] + rows[3]], axis=1))
        means.append(jnp.dot(jnp.concatenate(parts, axis=0), pick, precision=HI, preferred_element_type=F32))
    heatq = 1.0 + 0.1 * means[0]
    m = means[1]
    absorber = jnp.maximum(m, 0.0) + jnp.log1p(jnp.exp(-jnp.abs(m)))
    for q in range(4):
        for seg in range(2):
            at = pl.ds(4 * seg + q, 16, stride=8)
            low = q * LEV + 16 * seg
            arad[at, :] = absorber[low:low + 16]
            trad[at, :] = heatq[low:low + 16]
    tot_a = arad[0:8, :]
    for s in range(1, 16):
        tot_a = tot_a + arad[8 * s:8 * s + 8, :]
    a0s[...] = tot_a + roll(tot_a, 4, 0)

    fts[...] = flags_ref[...].astype(F32).T
    below = jnp.sum(fts[0:LEV, :], axis=0, keepdims=True)
    fsend[0:LEV, :] = fts[pl.ds(pl.multiple_of(LEV * og, 8), LEV), :]
    fsend[LEV:LEV + 8, :] = jnp.broadcast_to(below * (1.0 - gf), (8, 256))

    pl.semaphore_wait(barrier, len(peers))

    face = pl.multiple_of(PAD + 24 - 16 * g, 8)
    land = pl.multiple_of(PAD + 32 * g, 8)
    lev = pl.ds(own, LEV)
    sends = [
        copy(0, fsend, frecv, (og, x, y)),
        copy(1, a0s, a0r, (og, x, y)),
    ]
    for f in range(2):
        sends.append(copy(2 + f, fa.at[f, pl.ds(ROWS, H), lev, :], fa.at[f, pl.ds(0, H), lev, :], (g, xn, y)))
        sends.append(copy(4 + f, fa.at[f, pl.ds(H, H), lev, :], fa.at[f, pl.ds(H + ROWS, H), lev, :], (g, xp, y)))
    for f in range(2):
        sends.append(copy(6 + f, fa.at[f, pl.ds(H, ROWS), pl.ds(face, H), :], fa.at[f, pl.ds(H, ROWS), pl.ds(land, H), :], (og, x, y)))
        sends.append(copy(8 + f, fa.at[f, pl.ds(ROWS, H), pl.ds(face, H), :], fa.at[f, pl.ds(0, H), pl.ds(land, H), :], (og, xn, y)))
        sends.append(copy(10 + f, fa.at[f, pl.ds(H, H), pl.ds(face, H), :], fa.at[f, pl.ds(H + ROWS, H), pl.ds(land, H), :], (og, xp, y)))
    for c in sends:
        c.start()

    slot = lax.broadcasted_iota(jnp.int32, (512, COLS), 0)
    for q in range(4):
        line = jnp.concatenate([slot_ref[2 * q:2 * q + 1, :], slot_ref[2 * q + 1:2 * q + 2, :]], axis=1)
        oh[:, q * COLS:(q + 1) * COLS] = jnp.where(slot == line, 1.0, 0.0).astype(jnp.bfloat16)

    mine = pl.multiple_of(256 * g, 256)
    theirs = pl.multiple_of(256 * og, 256)
    fc[0:LEV, pl.ds(mine, 256)] = fts[pl.ds(pl.multiple_of(LEV * g, 8), LEV), :]
    fc[LEV:LEV + 8, pl.ds(mine, 256)] = jnp.broadcast_to(below * gf, (8, 256))
    sends[0].wait_recv()
    fc[:, pl.ds(theirs, 256)] = frecv[...]
    placed = jnp.dot(fc[...].astype(jnp.bfloat16), oh[...], preferred_element_type=F32)
    for q in range(4):
        part = placed[:, q * COLS:(q + 1) * COLS]
        for seg in range(2):
            crad[pl.ds(4 * seg + q, 16, stride=8), :] = part[16 * seg:16 * seg + 16]
            c0b[4 * seg + q:4 * seg + q + 1, :] = part[LEV:LEV + 1]
    tot_c = crad[0:8, :]
    for s in range(1, 16):
        tot_c = tot_c + crad[8 * s:8 * s + 8, :]
    second = subs((8, COLS)) >= 4
    sends[1].wait_recv()
    init_a = jnp.where(second, roll(tot_a, 4, 0), 0.0) + gf * a0r[...]
    init_c = jnp.where(second, roll(tot_c, 4, 0), 0.0) + c0b[...]
    a0r[...] = init_a
    c0b[...] = init_c

    scale = -math.log2(math.e)
    acc[...] = jnp.zeros_like(acc)

    def radiate(block, _):
        ks, ds, ls, beams = [], [], [], []
        start_a, start_c = a0r[...], c0b[...]
        for j in range(GB):
            n = block * GB + j
            ks.append(scale * k_ref[n])
            ds.append(scale * d_ref[n])
            ls.append(lw_ref[n])
            beams.append(sw_ref[n] * jnp.exp2(start_a * ks[j] + start_c * ds[j]))
        for s in range(16):
            a, c, q = (ref[8 * s:8 * s + 8, :] for ref in (arad, crad, trad))
            total = acc[8 * s:8 * s + 8, :]
            for j in range(GB):
                e = jnp.exp2(a * ks[j] + c * ds[j])
                total = total + (beams[j] - q * ls[j]) * (1.0 - e)
                beams[j] = beams[j] * e
            acc[8 * s:8 * s + 8, :] = total
        return 0

    lax.fori_loop(0, G // GB, radiate, 0)

    tiles = []
    for q in range(4):
        both = [acc[pl.ds(4 * seg + q, 16, stride=8), :] for seg in range(2)]
        tiles.append(jnp.concatenate(both, axis=0) * (4.0 / G))
    rates = jnp.concatenate(tiles, axis=1)
    stacked = jnp.concatenate(tiles, axis=0)

    kk = lax.broadcasted_iota(jnp.int32, (COLS, 2 * COLS), 0)
    nn = lax.broadcasted_iota(jnp.int32, (COLS, 2 * COLS), 1)
    same = (kk // 64) == (nn // COLS)
    col, src = nn % COLS, kk % 64
    up = jnp.where(src == col // 2, 0.75, jnp.where(src == col // 2 - 1 + 2 * (col % 2), 0.25, 0.0))
    up = jnp.where(same, up, 0.0).astype(F32)
    refined = jnp.dot(stacked, up, precision=HI, preferred_element_type=F32)
    lane = lanes((LEV, COLS))
    packed = jnp.zeros((LEV, COLS), F32)
    inner = []
    for i in range(8):
        q, half = i // 2, i % 2
        line = refined[q * LEV:(q + 1) * LEV, half * COLS:(half + 1) * COLS]
        inner.append(line)
        cus[1 + i] = line
        here = (lane == 2 * i) | (lane == (2 * i - 1) % COLS)
        packed = jnp.where(here, roll(line, 2 * i), packed)
    ews[...] = packed
    ends = [copy(12, ews, ewl, (g, x, yn)), copy(13, ews, ewr, (g, x, yp))]
    for c in ends:
        c.start()

    rest = rates
    total = None
    for _ in range(3):
        piece = rest.astype(jnp.bfloat16)
        rest = rest - piece.astype(F32)
        part = lax.dot_general(piece, oh[...], (((1,), (1,)), ((), ())), preferred_element_type=F32)
        total = part if total is None else total + part
    pws[...] = total
    back = copy(14, pws.at[:, pl.ds(theirs, 256)], wrecv, (og, x, y))
    back.start()
    wt[pl.ds(pl.multiple_of(LEV * g, 8), LEV), :] = pws[:, pl.ds(mine, 256)]

    for c in ends:
        c.wait_recv()
    left, right = ewl[...] * (1.0 / 3.0), ewr[...] * (1.0 / 3.0)
    for i in range(8):
        line = cus[1 + i]
        line = line + jnp.where(lane == 0, roll(left, 1 - 2 * i), 0.0)
        line = line + jnp.where(lane == COLS - 1, roll(right, COLS - 1 - 2 * i), 0.0)
        cus[1 + i] = line
    lines = [copy(15, cus.at[8], cus.at[0], (g, xn, y)), copy(16, cus.at[1], cus.at[9], (g, xp, y))]
    for c in lines:
        c.start()

    for c in sends[2:]:
        c.wait_recv()
    lane = lanes((XL, COLS))
    outer = (lane < 8) | (lane >= COLS - 8)
    ext = pl.ds(PAD, XL)

    def pack(t, _):
        total = None
        for j in range(4):
            row = 4 * t + j
            edge = jnp.where(outer, fa[0, row, ext, :], fa[1, row, ext, :])
            edge = roll(edge, 16 * j)
            seat = (lane + COLS + 8 - 16 * j) % 64 < 16
            total = edge if total is None else jnp.where(seat, edge, total)
        eps[t] = total
        return 0

    lax.fori_loop(0, XR // 4, pack, 0)
    edges = [copy(17, eps, epl, (g, x, yn)), copy(18, eps, epr, (g, x, yp))]
    for c in edges:
        c.start()
    for c in edges:
        c.wait_recv()
    from_left = (lane + 8) % 16 < 8

    def unpack(t, _):
        both = jnp.where(from_left, epl[t], epr[t])
        for j in range(4):
            ea[4 * t + j, ext, :] = roll(both, -16 * j)
        return 0

    lax.fori_loop(0, XR // 4, unpack, 0)
    for c in sends[2:]:
        c.wait_send()

    at_first, at_last = lane == 0, lane == COLS - 1
    mid_first, mid_last = lane == 64, lane == 63
    above, below_, = pl.ds(PAD - 1, XL), pl.ds(PAD + 1, XL)

    def step(src, esrc, r):
        an, ap, bn, bp = (coef[n] for n in range(4))

        def update(centre, nxt, prv, cols_n, cols_p, up_, down):
            return (
                (1.0 - 4.0 * NU_H - 2.0 * NU_V) * centre + an * nxt + ap * prv
                + bn * roll(cols_n, -1) + bp * roll(cols_p, 1) + NU_V * (up_ + down)
            )

        c0, c1, ce = src[0, r, ext, :], src[1, r, ext, :], esrc[r, ext, :]
        new0 = update(
            c0, src[0, r + 1, ext, :], src[0, r - 1, ext, :],
            jnp.where(at_first, ce, c0), jnp.where(at_last, ce, c0),
            src[0, r, above, :], src[0, r, below_, :],
        )
        new1 = update(
            c1, src[1, r + 1, ext, :], src[1, r - 1, ext, :],
            jnp.where(mid_first, ce, c1), jnp.where(mid_last, ce, c1),
            src[1, r, above, :], src[1, r, below_, :],
        )
        newe = update(
            ce, esrc[r + 1, ext, :], esrc[r - 1, ext, :],
            jnp.where(at_first, c0, jnp.where(mid_first, c1, ce)),
            jnp.where(at_last, c0, jnp.where(mid_last, c1, ce)),
            esrc[r, above, :], esrc[r, below_, :],
        )
        return new0, new1, newe

    bufs = [(fa, ea), (fb, eb)]
    for sweep in range(1, SWEEPS + 1):
        (src, esrc), (dst, edst) = bufs[(sweep - 1) % 2], bufs[sweep % 2]

        def row(r, _, src=src, esrc=esrc, dst=dst, edst=edst):
            new0, new1, newe = step(src, esrc, r)
            dst[0, r, ext, :] = new0
            dst[1, r, ext, :] = new1
            edst[r, ext, :] = newe
            return 0

        lax.fori_loop(sweep, XR - sweep, row, 0)

    for c in lines:
        c.wait_recv()

    def finish(i, _):
        for half in range(2):
            r = 2 * i + half
            heat = 0.75 * cus[1 + i] + 0.25 * cus[i + 2 * half]
            to_ref[pl.ds(r, LEV, stride=ROWS), :] = fa[0, H + r, pl.ds(own, LEV), :] + HEATING_INTERVAL * heat
            mo_ref[pl.ds(r, LEV, stride=ROWS), :] = roll(fa[1, H + r, pl.ds(own, LEV), :], 64)
        return 0

    lax.fori_loop(0, ROWS // 2, finish, 0)

    back.wait_recv()
    wt[pl.ds(pl.multiple_of(LEV * og, 8), LEV), :] = wrecv[...]
    wr_ref[...] = wt[...].T
    for c in [*sends[:2], *ends, back, *lines, *edges]:
        c.wait_send()


def body(sizes, t, m, cx, cy, k, d, sw, lw, flags, slots):
    smem = pl.BlockSpec(memory_space=pltpu.SMEM)
    vmem = pl.BlockSpec(memory_space=pltpu.VMEM)
    flat = (LEV * ROWS, COLS)
    scratch = [
        pltpu.VMEM((2, XR, ALL, COLS), F32),
        pltpu.VMEM((2, XR, ALL, COLS), F32),
        pltpu.VMEM((XR, ALL, COLS), F32),
        pltpu.VMEM((XR, ALL, COLS), F32),
        pltpu.VMEM((4, XL, COLS), F32),
        pltpu.VMEM((8, COLS), F32),
        pltpu.VMEM((128, COLS), F32),
        pltpu.VMEM((128, COLS), F32),
        pltpu.VMEM((128, COLS), F32),
        pltpu.VMEM((128, COLS), F32),
        pltpu.VMEM((2 * LEV, 256), F32),
        pltpu.VMEM((LEV + 8, 256), F32),
        pltpu.VMEM((LEV + 8, 256), F32),
        pltpu.VMEM((8, COLS), F32),
        pltpu.VMEM((8, COLS), F32),
        pltpu.VMEM((8, COLS), F32),
        pltpu.VMEM((512, 512), jnp.bfloat16),
        pltpu.VMEM((LEV + 8, 512), F32),
        pltpu.VMEM((LEV, 512), F32),
        pltpu.VMEM((LEV, 256), F32),
        pltpu.VMEM((2 * LEV, 256), F32),
        pltpu.VMEM((10, LEV, COLS), F32),
        pltpu.VMEM((LEV, COLS), F32),
        pltpu.VMEM((LEV, COLS), F32),
        pltpu.VMEM((LEV, COLS), F32),
        pltpu.VMEM((XR // 4, XL, COLS), F32),
        pltpu.VMEM((XR // 4, XL, COLS), F32),
        pltpu.VMEM((XR // 4, XL, COLS), F32),
        pltpu.SemaphoreType.DMA((19,)),
        pltpu.SemaphoreType.DMA((19,)),
    ]
    to, mo, wr = pl.pallas_call(
        functools.partial(kernel, sizes),
        out_shape=(
            jax.ShapeDtypeStruct(flat, F32),
            jax.ShapeDtypeStruct(flat, F32),
            jax.ShapeDtypeStruct((256, 2 * LEV), F32),
        ),
        in_specs=[smem] * 6 + [vmem] * 4,
        out_specs=(vmem, vmem, vmem),
        scratch_shapes=scratch,
        compiler_params=pltpu.CompilerParams(
            collective_id=0, has_side_effects=True, vmem_limit_bytes=32 * 1024 * 1024
        ),
    )(cx, cy, k, d, sw, lw, t.reshape(flat), m.reshape(flat), flags, slots)
    return to.reshape(t.shape), mo.reshape(t.shape), wr


def solution(mesh):
    sizes = tuple(mesh.shape[a] for a in ("grp", "gx", "gy"))
    in_specs = (
        P("grp", "gx", "gy"), P("grp", "gx", "gy"),
        P(), P(), P(), P(), P(), P(),
        P(("grp", "gx", "gy"), None), P("gx", "gy"),
    )
    out_specs = (P("grp", "gx", "gy"), P("grp", "gx", "gy"), P(("grp", "gx", "gy"), None))
    return jax.shard_map(
        functools.partial(body, sizes), mesh=mesh, in_specs=in_specs, out_specs=out_specs, check_vma=False
    )
```

```python
import functools
import math

import jax
import jax.numpy as jnp
from jax import lax
from jax.experimental import pallas as pl
from jax.experimental.pallas import tpu as pltpu
from jax.sharding import PartitionSpec as P

SWEEPS = 8
NU_H = 0.15
NU_V = 0.15
HEATING_INTERVAL = 0.5
LEV = 32
ROWS = 16
COLS = 128
H = 8
XR = ROWS + 2 * H
UP, OWN, DOWN, ALL = 8, 16, 48, 64
G = 112
GB = 4
F32 = jnp.float32
MESH = pl.DeviceIdType.MESH
HI = lax.Precision.HIGHEST


def lanes(shape):
    return lax.broadcasted_iota(jnp.int32, shape, len(shape) - 1)


def subs(shape):
    return lax.broadcasted_iota(jnp.int32, shape, len(shape) - 2)


def roll(x, amount, axis=1):
    n = x.shape[axis]
    amount = amount % n
    return x if amount == 0 else pltpu.roll(x, amount, axis)


def kernel(
    sizes,
    cx_hbm, cy_hbm, k_hbm, d_hbm, sw_hbm, lw_hbm,
    t_hbm, m_hbm, flags_hbm, slot_hbm,
    to_ref, mo_ref, wr_ref,
    cx_ref, cy_ref, k_ref, d_ref, sw_ref, lw_ref,
    tin, min_, fin, sin,
    fs, es, coef, arad, crad, trad, acc, fsend, frecv, a0r, c0b,
    oh, fc, pws, wrecv, cus, ews, ewl, ewr,
    eos, eol, eor, els, ell, elr, ehs, ehl, ehr, hst, hland,
    load, send, recv,
):
    ng, nx, ny = sizes
    g, x, y = lax.axis_index("grp"), lax.axis_index("gx"), lax.axis_index("gy")
    og = 1 - g
    xn, xp = lax.rem(x + 1, nx), lax.rem(x + nx - 1, nx)
    yn, yp = lax.rem(y + 1, ny), lax.rem(y + ny - 1, ny)
    gf = g.astype(F32)
    peers = [(og, x, y), (g, xn, y), (g, xp, y), (og, xn, y), (og, xp, y), (g, x, yn), (g, x, yp)]

    barrier = pltpu.get_barrier_semaphore()
    for peer in peers:
        pl.semaphore_signal(barrier, inc=1, device_id=peer, device_id_type=MESH)
    loads = [
        pltpu.make_async_copy(src, dst, load.at[n])
        for n, (src, dst) in enumerate((
            (m_hbm, min_), (t_hbm, tin), (flags_hbm, fin), (slot_hbm, sin), (cx_hbm, cx_ref),
            (cy_hbm, cy_ref), (k_hbm, k_ref), (d_hbm, d_ref), (sw_hbm, sw_ref), (lw_hbm, lw_ref),
        ))
    ]
    for c in loads:
        c.start()

    def copy(i, src, dst, peer):
        return pltpu.make_async_remote_copy(
            src_ref=src, dst_ref=dst, send_sem=send.at[i], recv_sem=recv.at[i],
            device_id=peer, device_id_type=MESH,
        )

    own = pl.ds(OWN, LEV)
    zero8 = jnp.zeros((8, COLS), F32)

    for c in loads[:2]:
        c.wait()

    def place(b, _):
        for j in range(4):
            r = 4 * b + j
            fs[0, 0, H + r, own, :] = tin[pl.ds(r, LEV, stride=ROWS), :]
            fs[0, 1, H + r, own, :] = roll(min_[pl.ds(r, LEV, stride=ROWS), :], 64)
        return 0

    lax.fori_loop(0, ROWS // 4, place, 0)
    for c in loads[2:]:
        c.wait()
    pl.semaphore_wait(barrier, len(peers))

    face = pl.ds(pl.multiple_of(DOWN - 8 - 24 * g, 8), H)
    land = pl.ds(pl.multiple_of(8 + 40 * g, 8), H)
    first, last, mid = pl.ds(H, H), pl.ds(ROWS, H), pl.ds(H, ROWS)
    low, high = pl.ds(0, H), pl.ds(H + ROWS, H)
    levels_in = [
        copy(4, fs.at[0, :, mid, face, :], fs.at[0, :, mid, land, :], (og, x, y)),
        copy(5, fs.at[0, :, last, face, :], fs.at[0, :, low, land, :], (og, xn, y)),
        copy(6, fs.at[0, :, first, face, :], fs.at[0, :, high, land, :], (og, xp, y)),
    ]
    rows_low = copy(2, fs.at[0, :, last, own, :], fs.at[0, :, low, own, :], (g, xn, y))
    rows_high = copy(3, hst, hland, (g, xp, y))
    for c in levels_in:
        c.start()

    for part in range(2):
        for r in range(H):
            hst[H * part + r] = fs[0, part, H + r, own, :]

    lane = lanes((LEV, COLS))
    outer = (lane < 8) | (lane >= COLS - 8)
    seats = [(lane + COLS + 8 - 16 * j) % 64 < 16 for j in range(4)]
    from_left = (lane + 8) % 16 < 8

    def pack(row, at=own, n=LEV):
        total = None
        for j in range(4):
            edge = jnp.where(outer[:n], fs[0, 0, row + j, at, :], fs[0, 1, row + j, at, :])
            edge = roll(edge, 16 * j)
            total = edge if total is None else jnp.where(seats[j][:n], edge, total)
        return total

    for t in range(4):
        eos[t] = pack(H + 4 * t)
    edges_own = [copy(7, eos, eol, (g, x, yn)), copy(8, eos, eor, (g, x, yp))]
    for c in edges_own:
        c.start()

    kk = lax.broadcasted_iota(jnp.int32, (2 * COLS, COLS), 0)
    nn = lax.broadcasted_iota(jnp.int32, (2 * COLS, COLS), 1)
    means = []
    for f in range(2):
        column = (kk + COLS - 64 * f) % COLS
        pick = jnp.where(nn == (kk // COLS) * 64 + column // 2, 0.25, 0.0).astype(F32)
        parts = []
        for q in range(4):
            rows = [fs[0, f, H + 4 * q + n, own, :] for n in range(4)]
            parts.append(jnp.concatenate([rows[0] + rows[1], rows[2] + rows[3]], axis=1))
        means.append(jnp.dot(jnp.concatenate(parts, axis=0), pick, precision=HI, preferred_element_type=F32))
    heatq = 1.0 + 0.1 * means[0]
    m = means[1]
    absorber = jnp.maximum(m, 0.0) + jnp.log1p(jnp.exp(-jnp.abs(m)))
    for q in range(4):
        for seg in range(2):
            at = pl.ds(4 * seg + q, 16, stride=8)
            low = q * LEV + 16 * seg
            arad[at, :] = absorber[low:low + 16]
            trad[at, :] = heatq[low:low + 16]
    tot_a = arad[0:8, :]
    for s in range(1, 16):
        tot_a = tot_a + arad[8 * s:8 * s + 8, :]
    below = jnp.sum(fin[0:LEV, :].astype(F32), axis=0, keepdims=True)
    whole_a = tot_a + roll(tot_a, 4, 0)
    fsend[0:LEV, :] = fin[pl.ds(pl.multiple_of(LEV * og, 8), LEV), :].astype(F32)
    fsend[LEV:LEV + 8, 0:COLS] = whole_a
    fsend[LEV:LEV + 8, COLS:2 * COLS] = whole_a
    fsend[LEV:LEV + 1, COLS:2 * COLS] = below[:, 0:COLS]
    fsend[LEV + 1:LEV + 2, COLS:2 * COLS] = below[:, COLS:256]
    clouds = copy(0, fsend, frecv, (og, x, y))
    for c in [clouds, rows_low]:
        c.start()

    for c in edges_own:
        c.wait_recv()
    for t in range(4):
        whole = jnp.where(from_left, eol[t], eor[t])
        if t < 2:
            hst[2 * H + t] = whole
        for j in range(4):
            es[0, H + 4 * t + j, own, :] = roll(whole, -16 * j)
    rows_high.start()

    dead = pl.ds(pl.multiple_of(8 + 40 * g, 8), H)
    zero8 = jnp.zeros((8, COLS), F32)

    def clear(r, _):
        for n in range(SWEEPS):
            for part in range(2):
                fs[n, part, r, dead, :] = zero8
            es[n, r, dead, :] = zero8
        return 0

    lax.fori_loop(0, XR, clear, 0)

    def coefs(i, _):
        level = i + 24 * g
        hx, hy = 0.5 * cx_ref[level], 0.5 * cy_ref[level]
        for n, value in enumerate((NU_H - hx, NU_H + hx, NU_H - hy, NU_H + hy)):
            coef[n, pl.ds(OWN - 8 * g + i, 1), :] = jnp.full((1, COLS), value, F32)
        return 0

    lax.fori_loop(0, LEV + H, coefs, 0)


    slot = lax.broadcasted_iota(jnp.int32, (512, COLS), 0)
    for q in range(4):
        line = jnp.concatenate([sin[2 * q:2 * q + 1, :], sin[2 * q + 1:2 * q + 2, :]], axis=1)
        oh[:, q * COLS:(q + 1) * COLS] = jnp.where(slot == line, 1.0, 0.0).astype(jnp.bfloat16)

    mine = pl.multiple_of(256 * g, 256)
    theirs = pl.multiple_of(256 * og, 256)
    def advance(sweep, lo, n, row0, count):
        here, above, beneath = pl.ds(lo, n), pl.ds(lo - 1, n), pl.ds(lo + 1, n)
        lane = lanes((n, COLS))
        at_first, at_last = lane == 0, lane == COLS - 1
        mid_first, mid_last = lane == 64, lane == 63
        p = sweep - 1
        an, ap, bn, bp = (coef[c, here, :] for c in range(4))

        def update(centre, nxt, prv, cols_n, cols_p, up_, down):
            return (
                (1.0 - 4.0 * NU_H - 2.0 * NU_V) * centre + an * nxt + ap * prv
                + bn * roll(cols_n, -1) + bp * roll(cols_p, 1) + NU_V * (up_ + down)
            )

        for j in range(count):
            r = row0 + j
            c0, c1, ce = fs[p, 0, r, here, :], fs[p, 1, r, here, :], es[p, r, here, :]
            fs[sweep, 0, r, here, :] = update(
                c0, fs[p, 0, r + 1, here, :], fs[p, 0, r - 1, here, :],
                jnp.where(at_first, ce, c0), jnp.where(at_last, ce, c0),
                fs[p, 0, r, above, :], fs[p, 0, r, beneath, :],
            )
            fs[sweep, 1, r, here, :] = update(
                c1, fs[p, 1, r + 1, here, :], fs[p, 1, r - 1, here, :],
                jnp.where(mid_first, ce, c1), jnp.where(mid_last, ce, c1),
                fs[p, 1, r, above, :], fs[p, 1, r, beneath, :],
            )
            es[sweep, r, here, :] = update(
                ce, es[p, r + 1, here, :], es[p, r - 1, here, :],
                jnp.where(at_first, c0, jnp.where(mid_first, c1, ce)),
                jnp.where(at_last, c0, jnp.where(mid_last, c1, ce)),
                es[p, r, above, :], es[p, r, beneath, :],
            )

    def blocks(sweep, lo, n, row0, count, each):
        def block(b, _):
            advance(sweep, lo, n, row0 + b * each, each)
            return 0

        lax.fori_loop(0, count // each, block, 0)

    clouds.wait_recv()
    fc[0:LEV, pl.ds(mine, 256)] = fin[pl.ds(pl.multiple_of(LEV * g, 8), LEV), :].astype(F32)
    fc[0:LEV, pl.ds(theirs, 256)] = frecv[0:LEV, :]
    fc[LEV:LEV + 8, pl.ds(mine, 256)] = jnp.broadcast_to(below * gf, (8, 256))
    count = jnp.concatenate([frecv[LEV:LEV + 1, COLS:256], frecv[LEV + 1:LEV + 2, COLS:256]], axis=1)
    fc[LEV:LEV + 8, pl.ds(theirs, 256)] = jnp.broadcast_to(count * gf, (8, 256))
    placed = jnp.dot(fc[...].astype(jnp.bfloat16), oh[...], preferred_element_type=F32)
    for q in range(4):
        part = placed[:, q * COLS:(q + 1) * COLS]
        for seg in range(2):
            crad[pl.ds(4 * seg + q, 16, stride=8), :] = part[16 * seg:16 * seg + 16]
            c0b[4 * seg + q:4 * seg + q + 1, :] = part[LEV:LEV + 1]
    tot_c = crad[0:8, :]
    for s in range(1, 16):
        tot_c = tot_c + crad[8 * s:8 * s + 8, :]
    second = subs((8, COLS)) >= 4
    init_a = jnp.where(second, roll(tot_a, 4, 0), 0.0) + gf * frecv[LEV:LEV + 8, 0:COLS]
    init_c = jnp.where(second, roll(tot_c, 4, 0), 0.0) + c0b[...]
    a0r[...] = init_a
    c0b[...] = init_c

    scale = -math.log2(math.e)
    acc[...] = jnp.zeros_like(acc)

    def radiate(block, _):
        ks, ds, ls, beams = [], [], [], []
        start_a, start_c = a0r[...], c0b[...]
        for j in range(GB):
            n = block * GB + j
            ks.append(scale * k_ref[n])
            ds.append(scale * d_ref[n])
            ls.append(lw_ref[n])
            beams.append(sw_ref[n] * jnp.exp2(start_a * ks[j] + start_c * ds[j]))
        for s in range(16):
            a, c, q = (ref[8 * s:8 * s + 8, :] for ref in (arad, crad, trad))
            total = acc[8 * s:8 * s + 8, :]
            for j in range(GB):
                e = jnp.exp2(a * ks[j] + c * ds[j])
                total = total + (beams[j] - q * ls[j]) * (1.0 - e)
                beams[j] = beams[j] * e
            acc[8 * s:8 * s + 8, :] = total
        return 0

    lax.fori_loop(0, G // GB, radiate, 0)

    tiles = []
    for q in range(4):
        both = [acc[pl.ds(4 * seg + q, 16, stride=8), :] for seg in range(2)]
        tiles.append(jnp.concatenate(both, axis=0) * (4.0 / G))
    rates = jnp.concatenate(tiles, axis=1)
    stacked = jnp.concatenate(tiles, axis=0)

    kk = lax.broadcasted_iota(jnp.int32, (COLS, 2 * COLS), 0)
    nn = lax.broadcasted_iota(jnp.int32, (COLS, 2 * COLS), 1)
    same = (kk // 64) == (nn // COLS)
    col, src = nn % COLS, kk % 64
    up = jnp.where(src == col // 2, 0.75, jnp.where(src == col // 2 - 1 + 2 * (col % 2), 0.25, 0.0))
    up = jnp.where(same, up, 0.0).astype(F32)
    refined = jnp.dot(stacked, up, precision=HI, preferred_element_type=F32)
    packed = jnp.zeros((LEV, COLS), F32)
    for i in range(8):
        q, half = i // 2, i % 2
        line = refined[q * LEV:(q + 1) * LEV, half * COLS:(half + 1) * COLS]
        cus[1 + i] = line
        here = (lane == 2 * i) | (lane == (2 * i - 1) % COLS)
        packed = jnp.where(here, roll(line, 2 * i), packed)
    ews[...] = packed
    ends = [copy(12, ews, ewl, (g, x, yn)), copy(13, ews, ewr, (g, x, yp))]
    for c in ends:
        c.start()

    rest = rates
    total = None
    for _ in range(3):
        piece = rest.astype(jnp.bfloat16)
        rest = rest - piece.astype(F32)
        part = lax.dot_general(piece, oh[...], (((1,), (1,)), ((), ())), preferred_element_type=F32)
        total = part if total is None else total + part
    pws[...] = total
    back = copy(14, pws.at[:, pl.ds(theirs, 256)], wrecv, (og, x, y))
    back.start()
    wr_ref[pl.ds(pl.multiple_of(LEV * g, 8), LEV), :] = pws[:, pl.ds(mine, 256)]

    for c in levels_in:
        c.wait_recv()
    arrived = pl.ds(pl.multiple_of(DOWN - 40 * g, 8), H)

    def pack_levels(t, _):
        els[t] = pack(4 * t, arrived, H)
        return 0

    lax.fori_loop(0, XR // 4, pack_levels, 0)
    edges_lev = [copy(1, els, ell, (g, x, yn)), copy(11, els, elr, (g, x, yp))]
    for c in edges_lev:
        c.start()

    edge_rows = []

    def offer():
        for t in range(2):
            ehs[t] = pack(4 * t)
        for i, dst, peer in ((9, ehl, (g, x, yn)), (10, ehr, (g, x, yp))):
            edge_rows.append(copy(i, ehs, dst, peer))
            edge_rows[-1].start()

    def take():
        for c in edge_rows:
            c.wait_recv()
        for t in range(2):
            whole = jnp.where(from_left, ehl[t], ehr[t])
            for j in range(4):
                es[0, 4 * t + j, own, :] = roll(whole, -16 * j)

    def sweep_side(n):
        for sweep in range(1, SWEEPS + 1):
            advance(sweep, lo, LEV + H, XR - sweep - H if n else sweep, H)

    rows_low.wait_recv()
    offer()

    for c in ends:
        c.wait_recv()
    left, right = ewl[...] * (1.0 / 3.0), ewr[...] * (1.0 / 3.0)
    for i in range(8):
        line = cus[1 + i]
        line = line + jnp.where(lane == 0, roll(left, 1 - 2 * i), 0.0)
        line = line + jnp.where(lane == COLS - 1, roll(right, COLS - 1 - 2 * i), 0.0)
        cus[1 + i] = line
    lines = [copy(15, cus.at[8], cus.at[0], (g, xn, y)), copy(16, cus.at[1], cus.at[9], (g, xp, y))]
    for c in lines:
        c.start()

    for c in edges_lev:
        c.wait_recv()

    def settle(t, _):
        whole = jnp.where(from_left[:H], ell[t], elr[t])
        for j in range(4):
            es[0, 4 * t + j, arrived, :] = roll(whole, -16 * j)
        return 0

    lax.fori_loop(0, XR // 4, settle, 0)
    lo = pl.multiple_of(OWN - 8 * g, 8)

    for sweep in range(1, SWEEPS):
        count = ROWS - 2 * sweep
        blocks(sweep, lo, LEV + H, H + sweep, count, {14: 7, 12: 6, 10: 5, 8: 4, 6: 6, 4: 4, 2: 2}[count])
    take()
    sweep_side(0)
    rows_high.wait_recv()
    for r in range(H):
        for part in range(2):
            fs[0, part, H + ROWS + r, own, :] = hland[H * part + r]
    for t in range(2):
        whole = hland[2 * H + t]
        for j in range(4):
            es[0, H + ROWS + 4 * t + j, own, :] = roll(whole, -16 * j)
    sweep_side(1)

    for c in lines:
        c.wait_recv()

    def finish(i, _):
        for half in range(2):
            r = 2 * i + half
            heat = 0.75 * cus[1 + i] + 0.25 * cus[i + 2 * half]
            to_ref[pl.ds(r, LEV, stride=ROWS), :] = fs[SWEEPS, 0, H + r, own, :] + HEATING_INTERVAL * heat
            mo_ref[pl.ds(r, LEV, stride=ROWS), :] = roll(fs[SWEEPS, 1, H + r, own, :], 64)
        return 0

    lax.fori_loop(0, ROWS // 2, finish, 0)

    back.wait_recv()
    wr_ref[pl.ds(pl.multiple_of(LEV * og, 8), LEV), :] = wrecv[...]
    for c in [clouds, rows_low, rows_high, *levels_in, *edges_own, *edge_rows, *edges_lev, *ends, back, *lines]:
        c.wait_send()


def write_out(*refs):
    copies = [pltpu.make_async_copy(refs[n], refs[3 + n], refs[6].at[n]) for n in range(3)]
    for c in copies:
        c.start()
    for c in copies:
        c.wait()


def body(sizes, t, m, cx, cy, k, d, sw, lw, flags, slots):
    vmem = pl.BlockSpec(memory_space=pltpu.VMEM)
    hbm = pl.BlockSpec(memory_space=pltpu.HBM)
    flat = (LEV * ROWS, COLS)
    scratch = [
        *[pltpu.SMEM((n,), F32) for n in (64, 64, G, G, G, G)],
        pltpu.VMEM(flat, F32),
        pltpu.VMEM(flat, F32),
        pltpu.VMEM((2 * LEV, 256), jnp.int32),
        pltpu.VMEM((8, 64), jnp.int32),
        pltpu.VMEM((SWEEPS + 1, 2, XR, ALL, COLS), F32),
        pltpu.VMEM((SWEEPS + 1, XR, ALL, COLS), F32),
        pltpu.VMEM((4, ALL, COLS), F32),
        pltpu.VMEM((128, COLS), F32),
        pltpu.VMEM((128, COLS), F32),
        pltpu.VMEM((128, COLS), F32),
        pltpu.VMEM((128, COLS), F32),
        pltpu.VMEM((LEV + 8, 256), F32),
        pltpu.VMEM((LEV + 8, 256), F32),
        pltpu.VMEM((8, COLS), F32),
        pltpu.VMEM((8, COLS), F32),
        pltpu.VMEM((512, 512), jnp.bfloat16),
        pltpu.VMEM((LEV + 8, 512), F32),
        pltpu.VMEM((LEV, 512), F32),
        pltpu.VMEM((LEV, 256), F32),
        pltpu.VMEM((10, LEV, COLS), F32),
        pltpu.VMEM((LEV, COLS), F32),
        pltpu.VMEM((LEV, COLS), F32),
        pltpu.VMEM((LEV, COLS), F32),
        pltpu.VMEM((4, LEV, COLS), F32),
        pltpu.VMEM((4, LEV, COLS), F32),
        pltpu.VMEM((4, LEV, COLS), F32),
        pltpu.VMEM((8, H, COLS), F32),
        pltpu.VMEM((8, H, COLS), F32),
        pltpu.VMEM((8, H, COLS), F32),
        pltpu.VMEM((2, LEV, COLS), F32),
        pltpu.VMEM((2, LEV, COLS), F32),
        pltpu.VMEM((2, LEV, COLS), F32),
        pltpu.VMEM((2 * H + 2, LEV, COLS), F32),
        pltpu.VMEM((2 * H + 2, LEV, COLS), F32),
        pltpu.SemaphoreType.DMA((10,)),
        pltpu.SemaphoreType.DMA((19,)),
        pltpu.SemaphoreType.DMA((19,)),
    ]
    to, mo, wr = pl.pallas_call(
        functools.partial(kernel, sizes),
        out_shape=(pltpu.VMEM(flat, F32), pltpu.VMEM(flat, F32), pltpu.VMEM((2 * LEV, 256), F32)),
        in_specs=[hbm] * 10,
        out_specs=(vmem, vmem, vmem),
        scratch_shapes=scratch,
        compiler_params=pltpu.CompilerParams(
            collective_id=0, has_side_effects=True, vmem_limit_bytes=67043328 - 640 * 1024
        ),
    )(cx, cy, k, d, sw, lw, t.reshape(flat), m.reshape(flat), flags.T, slots)
    to, mo, wr = pl.pallas_call(
        write_out,
        out_shape=tuple(jax.ShapeDtypeStruct(v.shape, F32) for v in (to, mo, wr)),
        in_specs=[vmem] * 3,
        out_specs=(hbm,) * 3,
        scratch_shapes=[pltpu.SemaphoreType.DMA((3,))],
        compiler_params=pltpu.CompilerParams(vmem_limit_bytes=1024 * 1024),
    )(to, mo, wr)
    return to.reshape(t.shape), mo.reshape(t.shape), wr.T


def solution(mesh):
    sizes = tuple(mesh.shape[a] for a in ("grp", "gx", "gy"))
    in_specs = (
        P("grp", "gx", "gy"), P("grp", "gx", "gy"),
        P(), P(), P(), P(), P(), P(),
        P(("grp", "gx", "gy"), None), P("gx", "gy"),
    )
    out_specs = (P("grp", "gx", "gy"), P("grp", "gx", "gy"), P(("grp", "gx", "gy"), None))
    return jax.shard_map(
        functools.partial(body, sizes), mesh=mesh, in_specs=in_specs, out_specs=out_specs, check_vma=False
    )
```

```python
import functools
import math

import jax
import jax.numpy as jnp
from jax import lax
from jax.experimental import pallas as pl
from jax.experimental.pallas import tpu as pltpu
from jax.sharding import PartitionSpec as P

SWEEPS = 8
NU_H = 0.15
NU_V = 0.15
HEATING_INTERVAL = 0.5
LEV = 32
ROWS = 16
COLS = 128
H = 8
XR = ROWS + 2 * H
UP, OWN, DOWN, ALL = 8, 16, 48, 64
G = 112
GB = 4
F32 = jnp.float32
MESH = pl.DeviceIdType.MESH
HI = lax.Precision.HIGHEST


def lanes(shape):
    return lax.broadcasted_iota(jnp.int32, shape, len(shape) - 1)


def subs(shape):
    return lax.broadcasted_iota(jnp.int32, shape, len(shape) - 2)


def roll(x, amount, axis=1):
    n = x.shape[axis]
    amount = amount % n
    return x if amount == 0 else pltpu.roll(x, amount, axis)


def kernel(
    sizes,
    cx_hbm, cy_hbm, k_hbm, d_hbm, sw_hbm, lw_hbm,
    t_hbm, m_hbm, flags_hbm, slot_hbm,
    to_ref, mo_ref, wr_ref,
    cx_ref, cy_ref, k_ref, d_ref, sw_ref, lw_ref,
    tin, min_, fin, sin,
    fs, es, coef, arad, crad, trad, acc, fsend, frecv, a0r, c0b,
    oh, fc, pws, wrecv, cus, ews, ewl, ewr,
    eos, eol, eor, els, ell, elr, ehs, ehl, ehr, hst, hland, cst, cland, lland,
    load, send, recv,
):
    ng, nx, ny = sizes
    g, x, y = lax.axis_index("grp"), lax.axis_index("gx"), lax.axis_index("gy")
    og = 1 - g
    xn, xp = lax.rem(x + 1, nx), lax.rem(x + nx - 1, nx)
    yn, yp = lax.rem(y + 1, ny), lax.rem(y + ny - 1, ny)
    gf = g.astype(F32)
    peers = [(og, x, y), (g, xn, y), (g, xp, y), (og, xn, y), (og, xp, y), (g, x, yn), (g, x, yp)]

    barrier = pltpu.get_barrier_semaphore()
    for peer in peers:
        pl.semaphore_signal(barrier, inc=1, device_id=peer, device_id_type=MESH)
    loads = [
        pltpu.make_async_copy(src, dst, load.at[n])
        for n, (src, dst) in enumerate((
            (m_hbm, min_), (t_hbm, tin), (flags_hbm, fin), (slot_hbm, sin), (cx_hbm, cx_ref),
            (cy_hbm, cy_ref), (k_hbm, k_ref), (d_hbm, d_ref), (sw_hbm, sw_ref), (lw_hbm, lw_ref),
        ))
    ]
    for c in loads:
        c.start()

    def copy(i, src, dst, peer):
        return pltpu.make_async_remote_copy(
            src_ref=src, dst_ref=dst, send_sem=send.at[i], recv_sem=recv.at[i],
            device_id=peer, device_id_type=MESH,
        )

    own = pl.ds(OWN, LEV)
    zero8 = jnp.zeros((8, COLS), F32)

    for c in loads[:2]:
        c.wait()

    def place(b, _):
        for j in range(4):
            r = 4 * b + j
            fs[0, 0, H + r, own, :] = tin[pl.ds(r, LEV, stride=ROWS), :]
            fs[0, 1, H + r, own, :] = roll(min_[pl.ds(r, LEV, stride=ROWS), :], 64)
        return 0

    lax.fori_loop(0, ROWS // 4, place, 0)
    for c in loads[2:]:
        c.wait()
    pl.semaphore_wait(barrier, len(peers))

    face = pl.ds(pl.multiple_of(DOWN - 8 - 24 * g, 8), H)
    first, last, mid = pl.ds(H, H), pl.ds(ROWS, H), pl.ds(H, ROWS)
    low, high = pl.ds(0, H), pl.ds(H + ROWS, H)
    levels_in = [
        copy(4, fs.at[0, :, mid, face, :], lland, (og, x, y)),
        copy(5, cst.at[0], cland.at[0], (og, xn, y)),
        copy(6, cst.at[1], cland.at[1], (og, xp, y)),
    ]
    rows_low = copy(2, fs.at[0, :, last, own, :], fs.at[0, :, low, own, :], (g, xn, y))
    rows_high = copy(3, hst, hland, (g, xp, y))
    levels_in[0].start()

    sub = subs((H, COLS))
    for n in range(2):
        for part in range(2):
            def row(d, n=n, part=part):
                return fs[0, part, 7 + d if n else 24 - d, face, :]

            for d in range(1, 4):
                first_group = jnp.where(sub >= d, row(d), roll(row(8 - d), d, 0))
                second_group = jnp.where(sub < 8 - d, row(d), roll(row(8 - d), 8 - d, 0))
                cst[n, 4 * part + d - 1] = jnp.where(g == 0, first_group, second_group)
            cst[n, 4 * part + 3] = row(4)
    for c in levels_in[1:]:
        c.start()

    for part in range(2):
        for r in range(H):
            hst[H * part + r] = fs[0, part, H + r, own, :]

    lane = lanes((LEV, COLS))
    outer = (lane < 8) | (lane >= COLS - 8)
    seats = [(lane + COLS + 8 - 16 * j) % 64 < 16 for j in range(4)]
    from_left = (lane + 8) % 16 < 8

    def pack(row, at=own, n=LEV):
        total = None
        for j in range(4):
            edge = jnp.where(outer[:n], fs[0, 0, row + j, at, :], fs[0, 1, row + j, at, :])
            edge = roll(edge, 16 * j)
            total = edge if total is None else jnp.where(seats[j][:n], edge, total)
        return total

    for t in range(4):
        eos[t] = pack(H + 4 * t)
    edges_own = [copy(7, eos, eol, (g, x, yn)), copy(8, eos, eor, (g, x, yp))]
    for c in edges_own:
        c.start()

    kk = lax.broadcasted_iota(jnp.int32, (2 * COLS, COLS), 0)
    nn = lax.broadcasted_iota(jnp.int32, (2 * COLS, COLS), 1)
    means = []
    for f in range(2):
        column = (kk + COLS - 64 * f) % COLS
        pick = jnp.where(nn == (kk // COLS) * 64 + column // 2, 0.25, 0.0).astype(F32)
        parts = []
        for q in range(4):
            rows = [fs[0, f, H + 4 * q + n, own, :] for n in range(4)]
            parts.append(jnp.concatenate([rows[0] + rows[1], rows[2] + rows[3]], axis=1))
        means.append(jnp.dot(jnp.concatenate(parts, axis=0), pick, precision=HI, preferred_element_type=F32))
    heatq = 1.0 + 0.1 * means[0]
    m = means[1]
    absorber = jnp.maximum(m, 0.0) + jnp.log1p(jnp.exp(-jnp.abs(m)))
    for q in range(4):
        for seg in range(2):
            at = pl.ds(4 * seg + q, 16, stride=8)
            low = q * LEV + 16 * seg
            arad[at, :] = absorber[low:low + 16]
            trad[at, :] = heatq[low:low + 16]
    tot_a = arad[0:8, :]
    for s in range(1, 16):
        tot_a = tot_a + arad[8 * s:8 * s + 8, :]
    below = jnp.sum(fin[0:LEV, :].astype(F32), axis=0, keepdims=True)
    whole_a = tot_a + roll(tot_a, 4, 0)
    fsend[0:LEV, :] = fin[pl.ds(pl.multiple_of(LEV * og, 8), LEV), :].astype(F32)
    fsend[LEV:LEV + 8, 0:COLS] = whole_a
    fsend[LEV:LEV + 8, COLS:2 * COLS] = whole_a
    fsend[LEV:LEV + 1, COLS:2 * COLS] = below[:, 0:COLS]
    fsend[LEV + 1:LEV + 2, COLS:2 * COLS] = below[:, COLS:256]
    clouds = copy(0, fsend, frecv, (og, x, y))
    for c in [clouds, rows_low]:
        c.start()

    for c in edges_own:
        c.wait_recv()
    for t in range(4):
        whole = jnp.where(from_left, eol[t], eor[t])
        if t < 2:
            hst[2 * H + t] = whole
        for j in range(4):
            es[0, H + 4 * t + j, own, :] = roll(whole, -16 * j)
    rows_high.start()

    zero8 = jnp.zeros((8, COLS), F32)

    def clear(r, _):
        for n in range(SWEEPS):
            for part in range(2):
                for side in (UP, DOWN):
                    fs[n, part, r, side:side + H, :] = zero8
            for side in (UP, DOWN):
                es[n, r, side:side + H, :] = zero8
        return 0

    lax.fori_loop(0, XR, clear, 0)

    def coefs(i, _):
        level = i + 24 * g
        hx, hy = 0.5 * cx_ref[level], 0.5 * cy_ref[level]
        for n, value in enumerate((NU_H - hx, NU_H + hx, NU_H - hy, NU_H + hy)):
            value = value * (1.0 / NU_V)
            coef[n, pl.ds(OWN - 8 * g + i, 1), :] = jnp.full((1, COLS), value, F32)
        return 0

    lax.fori_loop(0, LEV + H, coefs, 0)


    slot = lax.broadcasted_iota(jnp.int32, (512, COLS), 0)
    for q in range(4):
        line = jnp.concatenate([sin[2 * q:2 * q + 1, :], sin[2 * q + 1:2 * q + 2, :]], axis=1)
        oh[:, q * COLS:(q + 1) * COLS] = jnp.where(slot == line, 1.0, 0.0).astype(jnp.bfloat16)

    mine = pl.multiple_of(256 * g, 256)
    theirs = pl.multiple_of(256 * og, 256)
    def advance(sweep, lo, n, row0, count):
        here, above, beneath = pl.ds(lo, n), pl.ds(lo - 1, n), pl.ds(lo + 1, n)
        lane = lanes((n, COLS))
        at_first, at_last = lane == 0, lane == COLS - 1
        mid_first, mid_last = lane == 64, lane == 63
        p = sweep - 1
        an, ap, bn, bp = (coef[c, here, :] for c in range(4))

        def update(centre, nxt, prv, cols_n, cols_p, up_, down):
            return (
                ((1.0 - 4.0 * NU_H - 2.0 * NU_V) / NU_V) * centre + an * nxt + ap * prv
                + bn * roll(cols_n, -1) + bp * roll(cols_p, 1) + up_ + down
            )

        for j in range(count):
            r = row0 + j
            c0, c1, ce = fs[p, 0, r, here, :], fs[p, 1, r, here, :], es[p, r, here, :]
            fs[sweep, 0, r, here, :] = update(
                c0, fs[p, 0, r + 1, here, :], fs[p, 0, r - 1, here, :],
                jnp.where(at_first, ce, c0), jnp.where(at_last, ce, c0),
                fs[p, 0, r, above, :], fs[p, 0, r, beneath, :],
            )
            fs[sweep, 1, r, here, :] = update(
                c1, fs[p, 1, r + 1, here, :], fs[p, 1, r - 1, here, :],
                jnp.where(mid_first, ce, c1), jnp.where(mid_last, ce, c1),
                fs[p, 1, r, above, :], fs[p, 1, r, beneath, :],
            )
            es[sweep, r, here, :] = update(
                ce, es[p, r + 1, here, :], es[p, r - 1, here, :],
                jnp.where(at_first, c0, jnp.where(mid_first, c1, ce)),
                jnp.where(at_last, c0, jnp.where(mid_last, c1, ce)),
                es[p, r, above, :], es[p, r, beneath, :],
            )

    def blocks(sweep, lo, n, row0, count, each):
        def block(b, _):
            advance(sweep, lo, n, row0 + b * each, each)
            return 0

        lax.fori_loop(0, count // each, block, 0)

    lo = pl.multiple_of(OWN - 8 * g, 8)

    def inner_rows(at, n):
        for sweep in range(1, SWEEPS):
            count = ROWS - 2 * sweep
            blocks(sweep, at, n, H + sweep, count, {14: 7, 12: 6, 10: 5, 8: 4, 6: 6, 4: 4, 2: 2}[count])

    inner_rows(OWN, LEV)

    for c in levels_in:
        c.wait_recv()
    arrived = pl.ds(pl.multiple_of(DOWN - 40 * g, 8), H)

    for part in range(2):
        for r in range(ROWS):
            fs[0, part, H + r, arrived, :] = lland[part, r]
    for n in range(2):
        for part in range(2):
            def put(d, value, n=n, part=part):
                fs[0, part, 23 + d if n else 8 - d, arrived, :] = value

            for d in range(1, 4):
                both = cland[n, 4 * part + d - 1]
                put(d, both)
                put(8 - d, jnp.where(g == 1, roll(both, 8 - d, 0), roll(both, d, 0)))
            for d in (4, 8):
                put(d, cland[n, 4 * part + 3])

    def pack_levels(t, _):
        els[t] = pack(4 * t, arrived, H)
        return 0

    lax.fori_loop(0, XR // 4, pack_levels, 0)
    edges_lev = [copy(1, els, ell, (g, x, yn)), copy(11, els, elr, (g, x, yp))]
    for c in edges_lev:
        c.start()

    clouds.wait_recv()
    fc[0:LEV, pl.ds(mine, 256)] = fin[pl.ds(pl.multiple_of(LEV * g, 8), LEV), :].astype(F32)
    fc[0:LEV, pl.ds(theirs, 256)] = frecv[0:LEV, :]
    fc[LEV:LEV + 8, pl.ds(mine, 256)] = jnp.broadcast_to(below * gf, (8, 256))
    count = jnp.concatenate([frecv[LEV:LEV + 1, COLS:256], frecv[LEV + 1:LEV + 2, COLS:256]], axis=1)
    fc[LEV:LEV + 8, pl.ds(theirs, 256)] = jnp.broadcast_to(count * gf, (8, 256))
    placed = jnp.dot(fc[...].astype(jnp.bfloat16), oh[...], preferred_element_type=F32)
    for q in range(4):
        part = placed[:, q * COLS:(q + 1) * COLS]
        for seg in range(2):
            crad[pl.ds(4 * seg + q, 16, stride=8), :] = part[16 * seg:16 * seg + 16]
            c0b[4 * seg + q:4 * seg + q + 1, :] = part[LEV:LEV + 1]
    tot_c = crad[0:8, :]
    for s in range(1, 16):
        tot_c = tot_c + crad[8 * s:8 * s + 8, :]
    second = subs((8, COLS)) >= 4
    init_a = jnp.where(second, roll(tot_a, 4, 0), 0.0) + gf * frecv[LEV:LEV + 8, 0:COLS]
    init_c = jnp.where(second, roll(tot_c, 4, 0), 0.0) + c0b[...]
    a0r[...] = init_a
    c0b[...] = init_c

    scale = -math.log2(math.e)
    acc[...] = jnp.zeros_like(acc)

    def radiate(block, _):
        ks, ds, ls, beams = [], [], [], []
        start_a, start_c = a0r[...], c0b[...]
        for j in range(GB):
            n = block * GB + j
            ks.append(scale * k_ref[n])
            ds.append(scale * d_ref[n])
            ls.append(lw_ref[n])
            beams.append(sw_ref[n] * jnp.exp2(start_a * ks[j] + start_c * ds[j]))
        for s in range(16):
            a, c, q = (ref[8 * s:8 * s + 8, :] for ref in (arad, crad, trad))
            total = acc[8 * s:8 * s + 8, :]
            for j in range(GB):
                e = jnp.exp2(a * ks[j] + c * ds[j])
                total = total + (beams[j] - q * ls[j]) * (1.0 - e)
                beams[j] = beams[j] * e
            acc[8 * s:8 * s + 8, :] = total
        return 0

    lax.fori_loop(0, G // GB, radiate, 0)

    tiles = []
    for q in range(4):
        both = [acc[pl.ds(4 * seg + q, 16, stride=8), :] for seg in range(2)]
        tiles.append(jnp.concatenate(both, axis=0) * (4.0 / G))
    rates = jnp.concatenate(tiles, axis=1)
    stacked = jnp.concatenate(tiles, axis=0)

    kk = lax.broadcasted_iota(jnp.int32, (COLS, 2 * COLS), 0)
    nn = lax.broadcasted_iota(jnp.int32, (COLS, 2 * COLS), 1)
    same = (kk // 64) == (nn // COLS)
    col, src = nn % COLS, kk % 64
    up = jnp.where(src == col // 2, 0.75, jnp.where(src == col // 2 - 1 + 2 * (col % 2), 0.25, 0.0))
    up = jnp.where(same, up, 0.0).astype(F32)
    refined = jnp.dot(stacked, up, precision=HI, preferred_element_type=F32)
    packed = jnp.zeros((LEV, COLS), F32)
    for i in range(8):
        q, half = i // 2, i % 2
        line = refined[q * LEV:(q + 1) * LEV, half * COLS:(half + 1) * COLS]
        cus[1 + i] = line
        here = (lane == 2 * i) | (lane == (2 * i - 1) % COLS)
        packed = jnp.where(here, roll(line, 2 * i), packed)
    ews[...] = packed
    ends = [copy(12, ews, ewl, (g, x, yn)), copy(13, ews, ewr, (g, x, yp))]
    for c in ends:
        c.start()

    rest = rates
    total = None
    for _ in range(3):
        piece = rest.astype(jnp.bfloat16)
        rest = rest - piece.astype(F32)
        part = lax.dot_general(piece, oh[...], (((1,), (1,)), ((), ())), preferred_element_type=F32)
        total = part if total is None else total + part
    pws[...] = total
    back = copy(14, pws.at[:, pl.ds(theirs, 256)], wrecv, (og, x, y))
    back.start()
    wr_ref[pl.ds(pl.multiple_of(LEV * g, 8), LEV), :] = pws[:, pl.ds(mine, 256)]

    edge_rows = []

    def offer():
        for t in range(2):
            ehs[t] = pack(4 * t)
        for i, dst, peer in ((9, ehl, (g, x, yn)), (10, ehr, (g, x, yp))):
            edge_rows.append(copy(i, ehs, dst, peer))
            edge_rows[-1].start()

    def take():
        for c in edge_rows:
            c.wait_recv()
        for t in range(2):
            whole = jnp.where(from_left, ehl[t], ehr[t])
            for j in range(4):
                es[0, 4 * t + j, own, :] = roll(whole, -16 * j)

    def sweep_side(n):
        for sweep in range(1, SWEEPS + 1):
            advance(sweep, lo, LEV + H, XR - sweep - H if n else sweep, H)

    rows_low.wait_recv()
    offer()

    for c in ends:
        c.wait_recv()
    left, right = ewl[...] * (1.0 / 3.0), ewr[...] * (1.0 / 3.0)
    for i in range(8):
        line = cus[1 + i]
        line = line + jnp.where(lane == 0, roll(left, 1 - 2 * i), 0.0)
        line = line + jnp.where(lane == COLS - 1, roll(right, COLS - 1 - 2 * i), 0.0)
        cus[1 + i] = line
    lines = [copy(15, cus.at[8], cus.at[0], (g, xn, y)), copy(16, cus.at[1], cus.at[9], (g, xp, y))]
    for c in lines:
        c.start()

    for c in edges_lev:
        c.wait_recv()

    def settle(t, _):
        whole = jnp.where(from_left[:H], ell[t], elr[t])
        for j in range(4):
            es[0, 4 * t + j, arrived, :] = roll(whole, -16 * j)
        return 0

    lax.fori_loop(0, XR // 4, settle, 0)

    reach = pl.multiple_of(DOWN - 8 - 32 * g, 8)
    inner_rows(reach, 2 * H)
    take()
    sweep_side(0)
    rows_high.wait_recv()
    for r in range(H):
        for part in range(2):
            fs[0, part, H + ROWS + r, own, :] = hland[H * part + r]
    for t in range(2):
        whole = hland[2 * H + t]
        for j in range(4):
            es[0, H + ROWS + 4 * t + j, own, :] = roll(whole, -16 * j)
    sweep_side(1)

    for c in lines:
        c.wait_recv()

    def finish(i, _):
        for half in range(2):
            r = 2 * i + half
            heat = 0.75 * cus[1 + i] + 0.25 * cus[i + 2 * half]
            to_ref[pl.ds(r, LEV, stride=ROWS), :] = NU_V ** SWEEPS * fs[SWEEPS, 0, H + r, own, :] + HEATING_INTERVAL * heat
            mo_ref[pl.ds(r, LEV, stride=ROWS), :] = roll(NU_V ** SWEEPS * fs[SWEEPS, 1, H + r, own, :], 64)
        return 0

    lax.fori_loop(0, ROWS // 2, finish, 0)

    back.wait_recv()
    wr_ref[pl.ds(pl.multiple_of(LEV * og, 8), LEV), :] = wrecv[...]
    for c in [clouds, rows_low, rows_high, *levels_in, *edges_own, *edge_rows, *edges_lev, *ends, back, *lines]:
        c.wait_send()


def write_out(*refs):
    copies = [pltpu.make_async_copy(refs[n], refs[3 + n], refs[6].at[n]) for n in range(3)]
    for c in copies:
        c.start()
    for c in copies:
        c.wait()


def body(sizes, t, m, cx, cy, k, d, sw, lw, flags, slots):
    vmem = pl.BlockSpec(memory_space=pltpu.VMEM)
    hbm = pl.BlockSpec(memory_space=pltpu.HBM)
    flat = (LEV * ROWS, COLS)
    scratch = [
        *[pltpu.SMEM((n,), F32) for n in (64, 64, G, G, G, G)],
        pltpu.VMEM(flat, F32),
        pltpu.VMEM(flat, F32),
        pltpu.VMEM((2 * LEV, 256), jnp.int32),
        pltpu.VMEM((8, 64), jnp.int32),
        pltpu.VMEM((SWEEPS + 1, 2, XR, ALL, COLS), F32),
        pltpu.VMEM((SWEEPS + 1, XR, ALL, COLS), F32),
        pltpu.VMEM((4, ALL, COLS), F32),
        pltpu.VMEM((128, COLS), F32),
        pltpu.VMEM((128, COLS), F32),
        pltpu.VMEM((128, COLS), F32),
        pltpu.VMEM((128, COLS), F32),
        pltpu.VMEM((LEV + 8, 256), F32),
        pltpu.VMEM((LEV + 8, 256), F32),
        pltpu.VMEM((8, COLS), F32),
        pltpu.VMEM((8, COLS), F32),
        pltpu.VMEM((512, 512), jnp.bfloat16),
        pltpu.VMEM((LEV + 8, 512), F32),
        pltpu.VMEM((LEV, 512), F32),
        pltpu.VMEM((LEV, 256), F32),
        pltpu.VMEM((10, LEV, COLS), F32),
        pltpu.VMEM((LEV, COLS), F32),
        pltpu.VMEM((LEV, COLS), F32),
        pltpu.VMEM((LEV, COLS), F32),
        pltpu.VMEM((4, LEV, COLS), F32),
        pltpu.VMEM((4, LEV, COLS), F32),
        pltpu.VMEM((4, LEV, COLS), F32),
        pltpu.VMEM((8, H, COLS), F32),
        pltpu.VMEM((8, H, COLS), F32),
        pltpu.VMEM((8, H, COLS), F32),
        pltpu.VMEM((2, LEV, COLS), F32),
        pltpu.VMEM((2, LEV, COLS), F32),
        pltpu.VMEM((2, LEV, COLS), F32),
        pltpu.VMEM((2 * H + 2, LEV, COLS), F32),
        pltpu.VMEM((2 * H + 2, LEV, COLS), F32),
        pltpu.VMEM((2, 8, H, COLS), F32),
        pltpu.VMEM((2, 8, H, COLS), F32),
        pltpu.VMEM((2, ROWS, H, COLS), F32),
        pltpu.SemaphoreType.DMA((10,)),
        pltpu.SemaphoreType.DMA((19,)),
        pltpu.SemaphoreType.DMA((19,)),
    ]
    to, mo, wr = pl.pallas_call(
        functools.partial(kernel, sizes),
        out_shape=(pltpu.VMEM(flat, F32), pltpu.VMEM(flat, F32), pltpu.VMEM((2 * LEV, 256), F32)),
        in_specs=[hbm] * 10,
        out_specs=(vmem, vmem, vmem),
        scratch_shapes=scratch,
        compiler_params=pltpu.CompilerParams(
            collective_id=0, has_side_effects=True, vmem_limit_bytes=67043328 - 640 * 1024
        ),
    )(cx, cy, k, d, sw, lw, t.reshape(flat), m.reshape(flat), flags.T, slots)
    to, mo, wr = pl.pallas_call(
        write_out,
        out_shape=tuple(jax.ShapeDtypeStruct(v.shape, F32) for v in (to, mo, wr)),
        in_specs=[vmem] * 3,
        out_specs=(hbm,) * 3,
        scratch_shapes=[pltpu.SemaphoreType.DMA((3,))],
        compiler_params=pltpu.CompilerParams(vmem_limit_bytes=1024 * 1024),
    )(to, mo, wr)
    return to.reshape(t.shape), mo.reshape(t.shape), wr.T


def solution(mesh):
    sizes = tuple(mesh.shape[a] for a in ("grp", "gx", "gy"))
    in_specs = (
        P("grp", "gx", "gy"), P("grp", "gx", "gy"),
        P(), P(), P(), P(), P(), P(),
        P(("grp", "gx", "gy"), None), P("gx", "gy"),
    )
    out_specs = (P("grp", "gx", "gy"), P("grp", "gx", "gy"), P(("grp", "gx", "gy"), None))
    return jax.shard_map(
        functools.partial(body, sizes), mesh=mesh, in_specs=in_specs, out_specs=out_specs, check_vma=False
    )
```

```python
import functools
import math

import jax
import jax.numpy as jnp
from jax import lax
from jax.experimental import pallas as pl
from jax.experimental.pallas import tpu as pltpu
from jax.sharding import PartitionSpec as P

SWEEPS = 8
NU_H = 0.15
NU_V = 0.15
HEATING_INTERVAL = 0.5
LEV = 32
ROWS = 16
COLS = 128
H = 8
XR = ROWS + 2 * H
UP, OWN, DOWN, ALL = 8, 16, 48, 64
G = 112
GB = 4
F32 = jnp.float32
MESH = pl.DeviceIdType.MESH
HI = lax.Precision.HIGHEST


def lanes(shape):
    return lax.broadcasted_iota(jnp.int32, shape, len(shape) - 1)


def subs(shape):
    return lax.broadcasted_iota(jnp.int32, shape, len(shape) - 2)


def roll(x, amount, axis=1):
    n = x.shape[axis]
    amount = amount % n
    return x if amount == 0 else pltpu.roll(x, amount, axis)


def kernel(
    sizes,
    cx_hbm, cy_hbm, k_hbm, d_hbm, sw_hbm, lw_hbm,
    t_hbm, m_hbm, flags_hbm, slot_hbm,
    to_ref, mo_ref, wr_ref,
    cx_ref, cy_ref, k_ref, d_ref, sw_ref, lw_ref,
    tin, min_, fin, sin,
    fs, es, coef, arad, crad, trad, acc, fsend, frecv, a0r, c0b,
    oh, fc, pws, wrecv, cus, ews, ewl, ewr,
    eos, eol, eor, els, ell, elr, hst, hland, cst, cland, lland,
    load, send, recv,
):
    ng, nx, ny = sizes
    g, x, y = lax.axis_index("grp"), lax.axis_index("gx"), lax.axis_index("gy")
    og = 1 - g
    xn, xp = lax.rem(x + 1, nx), lax.rem(x + nx - 1, nx)
    yn, yp = lax.rem(y + 1, ny), lax.rem(y + ny - 1, ny)
    gf = g.astype(F32)
    peers = [(og, x, y), (g, xn, y), (g, xp, y), (og, xn, y), (og, xp, y), (g, x, yn), (g, x, yp)]

    barrier = pltpu.get_barrier_semaphore()
    for peer in peers:
        pl.semaphore_signal(barrier, inc=1, device_id=peer, device_id_type=MESH)
    loads = [
        pltpu.make_async_copy(src, dst, load.at[n])
        for n, (src, dst) in enumerate((
            (m_hbm, min_), (t_hbm, tin), (flags_hbm, fin), (slot_hbm, sin), (cx_hbm, cx_ref),
            (cy_hbm, cy_ref), (k_hbm, k_ref), (d_hbm, d_ref), (sw_hbm, sw_ref), (lw_hbm, lw_ref),
        ))
    ]
    for c in loads:
        c.start()

    def copy(i, src, dst, peer):
        return pltpu.make_async_remote_copy(
            src_ref=src, dst_ref=dst, send_sem=send.at[i], recv_sem=recv.at[i],
            device_id=peer, device_id_type=MESH,
        )

    own = pl.ds(OWN, LEV)
    zero8 = jnp.zeros((8, COLS), F32)

    for c in loads[:2]:
        c.wait()

    def place(b, _):
        for j in range(4):
            r = 4 * b + j
            fs[0, 0, H + r, own, :] = tin[pl.ds(r, LEV, stride=ROWS), :]
            fs[0, 1, H + r, own, :] = roll(min_[pl.ds(r, LEV, stride=ROWS), :], 64)
        return 0

    lax.fori_loop(0, ROWS // 4, place, 0)
    for c in loads[2:]:
        c.wait()
    pl.semaphore_wait(barrier, len(peers))

    face = pl.ds(pl.multiple_of(DOWN - 8 - 24 * g, 8), H)
    mid = pl.ds(H, ROWS)
    levels_in = [
        copy(4, fs.at[0, :, mid, face, :], lland, (og, x, y)),
        copy(5, cst.at[0], cland.at[0], (og, xn, y)),
        copy(6, cst.at[1], cland.at[1], (og, xp, y)),
    ]
    rows_low = copy(2, hst.at[0], hland.at[0], (g, xn, y))
    rows_high = copy(3, hst.at[1], hland.at[1], (g, xp, y))

    sub = subs((H, COLS))
    for n in range(2):
        for part in range(2):
            def row(d, n=n, part=part):
                return fs[0, part, 7 + d if n else 24 - d, face, :]

            for d in range(1, 4):
                first_group = jnp.where(sub >= d, row(d), roll(row(8 - d), d, 0))
                second_group = jnp.where(sub < 8 - d, row(d), roll(row(8 - d), 8 - d, 0))
                cst[n, 4 * part + d - 1] = jnp.where(g == 0, first_group, second_group)
            cst[n, 4 * part + 3] = row(4)
    for c in levels_in[1:]:
        c.start()

    for part in range(2):
        for r in range(H):
            hst[0, H * part + r] = fs[0, part, ROWS + r, own, :]
            hst[1, H * part + r] = fs[0, part, H + r, own, :]

    lane = lanes((LEV, COLS))
    outer = (lane < 8) | (lane >= COLS - 8)
    seats = [(lane + COLS + 8 - 16 * j) % 64 < 16 for j in range(4)]
    from_left = (lane + 8) % 16 < 8

    def pack(row, at=own, n=LEV):
        total = None
        for j in range(4):
            edge = jnp.where(outer[:n], fs[0, 0, row + j, at, :], fs[0, 1, row + j, at, :])
            edge = roll(edge, 16 * j)
            total = edge if total is None else jnp.where(seats[j][:n], edge, total)
        return total

    for t in range(4):
        eos[t] = pack(H + 4 * t)
    edges_own = [copy(7, eos, eol, (g, x, yn)), copy(8, eos, eor, (g, x, yp))]
    for c in edges_own:
        c.start()

    kk = lax.broadcasted_iota(jnp.int32, (2 * COLS, COLS), 0)
    nn = lax.broadcasted_iota(jnp.int32, (2 * COLS, COLS), 1)
    means = []
    for f in range(2):
        column = (kk + COLS - 64 * f) % COLS
        pick = jnp.where(nn == (kk // COLS) * 64 + column // 2, 0.25, 0.0).astype(F32)
        parts = []
        for q in range(4):
            rows = [fs[0, f, H + 4 * q + n, own, :] for n in range(4)]
            parts.append(jnp.concatenate([rows[0] + rows[1], rows[2] + rows[3]], axis=1))
        means.append(jnp.dot(jnp.concatenate(parts, axis=0), pick, precision=HI, preferred_element_type=F32))
    heatq = 1.0 + 0.1 * means[0]
    m = means[1]
    absorber = jnp.maximum(m, 0.0) + jnp.log1p(jnp.exp(-jnp.abs(m)))
    for q in range(4):
        for seg in range(2):
            at = pl.ds(4 * seg + q, 16, stride=8)
            low = q * LEV + 16 * seg
            arad[at, :] = absorber[low:low + 16]
            trad[at, :] = heatq[low:low + 16]
    tot_a = arad[0:8, :]
    for s in range(1, 16):
        tot_a = tot_a + arad[8 * s:8 * s + 8, :]
    below = jnp.sum(fin[0:LEV, :].astype(F32), axis=0, keepdims=True)
    whole_a = tot_a + roll(tot_a, 4, 0)
    fsend[0:LEV, :] = fin[pl.ds(pl.multiple_of(LEV * og, 8), LEV), :].astype(F32)
    fsend[LEV:LEV + 8, 0:COLS] = whole_a
    fsend[LEV:LEV + 8, COLS:2 * COLS] = whole_a
    fsend[LEV:LEV + 1, COLS:2 * COLS] = below[:, 0:COLS]
    fsend[LEV + 1:LEV + 2, COLS:2 * COLS] = below[:, COLS:256]
    clouds = copy(0, fsend, frecv, (og, x, y))
    for c in [clouds, levels_in[0]]:
        c.start()

    for c in edges_own:
        c.wait_recv()
    for t in range(4):
        whole = jnp.where(from_left, eol[t], eor[t])
        hst[1 - t // 2, 2 * H + t % 2] = whole
        for j in range(4):
            es[0, H + 4 * t + j, own, :] = roll(whole, -16 * j)
    for c in (rows_low, rows_high):
        c.start()

    zero8 = jnp.zeros((8, COLS), F32)

    def clear(r, _):
        for n in range(SWEEPS):
            for part in range(2):
                for side in (UP, DOWN):
                    fs[n, part, r, side:side + H, :] = zero8
            for side in (UP, DOWN):
                es[n, r, side:side + H, :] = zero8
        return 0

    lax.fori_loop(0, XR, clear, 0)

    def coefs(i, _):
        level = i + 24 * g
        hx, hy = 0.5 * cx_ref[level], 0.5 * cy_ref[level]
        for n, value in enumerate((NU_H - hx, NU_H + hx, NU_H - hy, NU_H + hy)):
            value = value * (1.0 / NU_V)
            coef[n, pl.ds(OWN - 8 * g + i, 1), :] = jnp.full((1, COLS), value, F32)
        return 0

    lax.fori_loop(0, LEV + H, coefs, 0)


    slot = lax.broadcasted_iota(jnp.int32, (512, COLS), 0)
    for q in range(4):
        line = jnp.concatenate([sin[2 * q:2 * q + 1, :], sin[2 * q + 1:2 * q + 2, :]], axis=1)
        oh[:, q * COLS:(q + 1) * COLS] = jnp.where(slot == line, 1.0, 0.0).astype(jnp.bfloat16)

    mine = pl.multiple_of(256 * g, 256)
    theirs = pl.multiple_of(256 * og, 256)
    def advance(sweep, lo, n, row0, count):
        here, above, beneath = pl.ds(lo, n), pl.ds(lo - 1, n), pl.ds(lo + 1, n)
        lane = lanes((n, COLS))
        at_first, at_last = lane == 0, lane == COLS - 1
        mid_first, mid_last = lane == 64, lane == 63
        p = sweep - 1
        an, ap, bn, bp = (coef[c, here, :] for c in range(4))

        def update(centre, nxt, prv, cols_n, cols_p, up_, down):
            return (
                ((1.0 - 4.0 * NU_H - 2.0 * NU_V) / NU_V) * centre + an * nxt + ap * prv
                + bn * roll(cols_n, -1) + bp * roll(cols_p, 1) + up_ + down
            )

        for j in range(count):
            r = row0 + j
            c0, c1, ce = fs[p, 0, r, here, :], fs[p, 1, r, here, :], es[p, r, here, :]
            fs[sweep, 0, r, here, :] = update(
                c0, fs[p, 0, r + 1, here, :], fs[p, 0, r - 1, here, :],
                jnp.where(at_first, ce, c0), jnp.where(at_last, ce, c0),
                fs[p, 0, r, above, :], fs[p, 0, r, beneath, :],
            )
            fs[sweep, 1, r, here, :] = update(
                c1, fs[p, 1, r + 1, here, :], fs[p, 1, r - 1, here, :],
                jnp.where(mid_first, ce, c1), jnp.where(mid_last, ce, c1),
                fs[p, 1, r, above, :], fs[p, 1, r, beneath, :],
            )
            es[sweep, r, here, :] = update(
                ce, es[p, r + 1, here, :], es[p, r - 1, here, :],
                jnp.where(at_first, c0, jnp.where(mid_first, c1, ce)),
                jnp.where(at_last, c0, jnp.where(mid_last, c1, ce)),
                es[p, r, above, :], es[p, r, beneath, :],
            )

    def blocks(sweep, lo, n, row0, count, each):
        def block(b, _):
            advance(sweep, lo, n, row0 + b * each, each)
            return 0

        lax.fori_loop(0, count // each, block, 0)

    lo = pl.multiple_of(OWN - 8 * g, 8)

    def inner_rows(at, n):
        for sweep in range(1, SWEEPS):
            count = ROWS - 2 * sweep
            blocks(sweep, at, n, H + sweep, count, {14: 7, 12: 6, 10: 5, 8: 4, 6: 6, 4: 4, 2: 2}[count])

    inner_rows(OWN, LEV)

    clouds.wait_recv()
    fc[0:LEV, pl.ds(mine, 256)] = fin[pl.ds(pl.multiple_of(LEV * g, 8), LEV), :].astype(F32)
    fc[0:LEV, pl.ds(theirs, 256)] = frecv[0:LEV, :]
    fc[LEV:LEV + 8, pl.ds(mine, 256)] = jnp.broadcast_to(below * gf, (8, 256))
    count = jnp.concatenate([frecv[LEV:LEV + 1, COLS:256], frecv[LEV + 1:LEV + 2, COLS:256]], axis=1)
    fc[LEV:LEV + 8, pl.ds(theirs, 256)] = jnp.broadcast_to(count * gf, (8, 256))
    placed = jnp.dot(fc[...].astype(jnp.bfloat16), oh[...], preferred_element_type=F32)
    for q in range(4):
        part = placed[:, q * COLS:(q + 1) * COLS]
        for seg in range(2):
            crad[pl.ds(4 * seg + q, 16, stride=8), :] = part[16 * seg:16 * seg + 16]
            c0b[4 * seg + q:4 * seg + q + 1, :] = part[LEV:LEV + 1]
    tot_c = crad[0:8, :]
    for s in range(1, 16):
        tot_c = tot_c + crad[8 * s:8 * s + 8, :]
    second = subs((8, COLS)) >= 4
    init_a = jnp.where(second, roll(tot_a, 4, 0), 0.0) + gf * frecv[LEV:LEV + 8, 0:COLS]
    init_c = jnp.where(second, roll(tot_c, 4, 0), 0.0) + c0b[...]
    a0r[...] = init_a
    c0b[...] = init_c

    scale = -math.log2(math.e)
    acc[...] = jnp.zeros_like(acc)

    def radiate(block, _):
        ks, ds, ls, beams = [], [], [], []
        start_a, start_c = a0r[...], c0b[...]
        for j in range(GB):
            n = block * GB + j
            ks.append(scale * k_ref[n])
            ds.append(scale * d_ref[n])
            ls.append(lw_ref[n])
            beams.append(sw_ref[n] * jnp.exp2(start_a * ks[j] + start_c * ds[j]))
        for s in range(16):
            a, c, q = (ref[8 * s:8 * s + 8, :] for ref in (arad, crad, trad))
            total = acc[8 * s:8 * s + 8, :]
            for j in range(GB):
                e = jnp.exp2(a * ks[j] + c * ds[j])
                total = total + (beams[j] - q * ls[j]) * (1.0 - e)
                beams[j] = beams[j] * e
            acc[8 * s:8 * s + 8, :] = total
        return 0

    lax.fori_loop(0, G // GB, radiate, 0)

    tiles = []
    for q in range(4):
        both = [acc[pl.ds(4 * seg + q, 16, stride=8), :] for seg in range(2)]
        tiles.append(jnp.concatenate(both, axis=0) * (4.0 / G))
    rates = jnp.concatenate(tiles, axis=1)
    stacked = jnp.concatenate(tiles, axis=0)

    kk = lax.broadcasted_iota(jnp.int32, (COLS, 2 * COLS), 0)
    nn = lax.broadcasted_iota(jnp.int32, (COLS, 2 * COLS), 1)
    same = (kk // 64) == (nn // COLS)
    col, src = nn % COLS, kk % 64
    up = jnp.where(src == col // 2, 0.75, jnp.where(src == col // 2 - 1 + 2 * (col % 2), 0.25, 0.0))
    up = jnp.where(same, up, 0.0).astype(F32)
    refined = jnp.dot(stacked, up, precision=HI, preferred_element_type=F32)
    packed = jnp.zeros((LEV, COLS), F32)
    for i in range(8):
        q, half = i // 2, i % 2
        line = refined[q * LEV:(q + 1) * LEV, half * COLS:(half + 1) * COLS]
        cus[1 + i] = line
        here = (lane == 2 * i) | (lane == (2 * i - 1) % COLS)
        packed = jnp.where(here, roll(line, 2 * i), packed)
    ews[...] = packed
    ends = [copy(12, ews, ewl, (g, x, yn)), copy(13, ews, ewr, (g, x, yp))]
    for c in ends:
        c.start()

    rest = rates
    total = None
    for _ in range(3):
        piece = rest.astype(jnp.bfloat16)
        rest = rest - piece.astype(F32)
        part = lax.dot_general(piece, oh[...], (((1,), (1,)), ((), ())), preferred_element_type=F32)
        total = part if total is None else total + part
    pws[...] = total
    back = copy(14, pws.at[:, pl.ds(theirs, 256)], wrecv, (og, x, y))
    wr_ref[pl.ds(pl.multiple_of(LEV * g, 8), LEV), :] = pws[:, pl.ds(mine, 256)]

    for c in levels_in:
        c.wait_recv()
    arrived = pl.ds(pl.multiple_of(DOWN - 40 * g, 8), H)

    for part in range(2):
        for r in range(ROWS):
            fs[0, part, H + r, arrived, :] = lland[part, r]
    for n in range(2):
        for part in range(2):
            def put(d, value, n=n, part=part):
                fs[0, part, 23 + d if n else 8 - d, arrived, :] = value

            for d in range(1, 4):
                both = cland[n, 4 * part + d - 1]
                put(d, both)
                put(8 - d, jnp.where(g == 1, roll(both, 8 - d, 0), roll(both, d, 0)))
            for d in (4, 8):
                put(d, cland[n, 4 * part + 3])

    def pack_levels(t, _):
        els[t] = pack(4 * t, arrived, H)
        return 0

    lax.fori_loop(0, XR // 4, pack_levels, 0)
    edges_lev = [copy(1, els, ell, (g, x, yn)), copy(11, els, elr, (g, x, yp))]
    for c in edges_lev:
        c.start()

    def take(n):
        for r in range(H):
            for part in range(2):
                fs[0, part, n * (H + ROWS) + r, own, :] = hland[n, H * part + r]
        for t in range(2):
            whole = hland[n, 2 * H + t]
            for j in range(4):
                es[0, n * (H + ROWS) + 4 * t + j, own, :] = roll(whole, -16 * j)

    def sweep_side(n):
        for sweep in range(1, SWEEPS + 1):
            advance(sweep, lo, LEV + H, XR - sweep - H if n else sweep, H)


    for c in ends:
        c.wait_recv()
    left, right = ewl[...] * (1.0 / 3.0), ewr[...] * (1.0 / 3.0)
    for i in range(8):
        line = cus[1 + i]
        line = line + jnp.where(lane == 0, roll(left, 1 - 2 * i), 0.0)
        line = line + jnp.where(lane == COLS - 1, roll(right, COLS - 1 - 2 * i), 0.0)
        cus[1 + i] = line
    lines = [copy(15, cus.at[8], cus.at[0], (g, xn, y)), copy(16, cus.at[1], cus.at[9], (g, xp, y))]
    for c in [*lines, back]:
        c.start()

    for c in edges_lev:
        c.wait_recv()

    def settle(t, _):
        whole = jnp.where(from_left[:H], ell[t], elr[t])
        for j in range(4):
            es[0, 4 * t + j, arrived, :] = roll(whole, -16 * j)
        return 0

    lax.fori_loop(0, XR // 4, settle, 0)

    reach = pl.multiple_of(DOWN - 8 - 32 * g, 8)
    inner_rows(reach, 2 * H)
    rows_low.wait_recv()
    take(0)
    sweep_side(0)
    rows_high.wait_recv()
    take(1)
    sweep_side(1)

    for c in lines:
        c.wait_recv()

    def finish(i, _):
        for half in range(2):
            r = 2 * i + half
            heat = 0.75 * cus[1 + i] + 0.25 * cus[i + 2 * half]
            to_ref[pl.ds(r, LEV, stride=ROWS), :] = NU_V ** SWEEPS * fs[SWEEPS, 0, H + r, own, :] + HEATING_INTERVAL * heat
            mo_ref[pl.ds(r, LEV, stride=ROWS), :] = roll(NU_V ** SWEEPS * fs[SWEEPS, 1, H + r, own, :], 64)
        return 0

    lax.fori_loop(0, ROWS // 2, finish, 0)

    back.wait_recv()
    wr_ref[pl.ds(pl.multiple_of(LEV * og, 8), LEV), :] = wrecv[...]
    for c in [clouds, rows_low, rows_high, *levels_in, *edges_own, *edges_lev, *ends, back, *lines]:
        c.wait_send()


def write_out(*refs):
    copies = [pltpu.make_async_copy(refs[n], refs[3 + n], refs[6].at[n]) for n in range(3)]
    for c in copies:
        c.start()
    for c in copies:
        c.wait()


def body(sizes, t, m, cx, cy, k, d, sw, lw, flags, slots):
    vmem = pl.BlockSpec(memory_space=pltpu.VMEM)
    hbm = pl.BlockSpec(memory_space=pltpu.HBM)
    flat = (LEV * ROWS, COLS)
    scratch = [
        *[pltpu.SMEM((n,), F32) for n in (64, 64, G, G, G, G)],
        pltpu.VMEM(flat, F32),
        pltpu.VMEM(flat, F32),
        pltpu.VMEM((2 * LEV, 256), jnp.int32),
        pltpu.VMEM((8, 64), jnp.int32),
        pltpu.VMEM((SWEEPS + 1, 2, XR, ALL, COLS), F32),
        pltpu.VMEM((SWEEPS + 1, XR, ALL, COLS), F32),
        pltpu.VMEM((4, ALL, COLS), F32),
        pltpu.VMEM((128, COLS), F32),
        pltpu.VMEM((128, COLS), F32),
        pltpu.VMEM((128, COLS), F32),
        pltpu.VMEM((128, COLS), F32),
        pltpu.VMEM((LEV + 8, 256), F32),
        pltpu.VMEM((LEV + 8, 256), F32),
        pltpu.VMEM((8, COLS), F32),
        pltpu.VMEM((8, COLS), F32),
        pltpu.VMEM((512, 512), jnp.bfloat16),
        pltpu.VMEM((LEV + 8, 512), F32),
        pltpu.VMEM((LEV, 512), F32),
        pltpu.VMEM((LEV, 256), F32),
        pltpu.VMEM((10, LEV, COLS), F32),
        pltpu.VMEM((LEV, COLS), F32),
        pltpu.VMEM((LEV, COLS), F32),
        pltpu.VMEM((LEV, COLS), F32),
        pltpu.VMEM((4, LEV, COLS), F32),
        pltpu.VMEM((4, LEV, COLS), F32),
        pltpu.VMEM((4, LEV, COLS), F32),
        pltpu.VMEM((8, H, COLS), F32),
        pltpu.VMEM((8, H, COLS), F32),
        pltpu.VMEM((8, H, COLS), F32),
        pltpu.VMEM((2, 2 * H + 2, LEV, COLS), F32),
        pltpu.VMEM((2, 2 * H + 2, LEV, COLS), F32),
        pltpu.VMEM((2, 8, H, COLS), F32),
        pltpu.VMEM((2, 8, H, COLS), F32),
        pltpu.VMEM((2, ROWS, H, COLS), F32),
        pltpu.SemaphoreType.DMA((10,)),
        pltpu.SemaphoreType.DMA((19,)),
        pltpu.SemaphoreType.DMA((19,)),
    ]
    to, mo, wr = pl.pallas_call(
        functools.partial(kernel, sizes),
        out_shape=(pltpu.VMEM(flat, F32), pltpu.VMEM(flat, F32), pltpu.VMEM((2 * LEV, 256), F32)),
        in_specs=[hbm] * 10,
        out_specs=(vmem, vmem, vmem),
        scratch_shapes=scratch,
        compiler_params=pltpu.CompilerParams(
            collective_id=0, has_side_effects=True, vmem_limit_bytes=67043328 - 640 * 1024
        ),
    )(cx, cy, k, d, sw, lw, t.reshape(flat), m.reshape(flat), flags.T, slots)
    to, mo, wr = pl.pallas_call(
        write_out,
        out_shape=tuple(jax.ShapeDtypeStruct(v.shape, F32) for v in (to, mo, wr)),
        in_specs=[vmem] * 3,
        out_specs=(hbm,) * 3,
        scratch_shapes=[pltpu.SemaphoreType.DMA((3,))],
        compiler_params=pltpu.CompilerParams(vmem_limit_bytes=1024 * 1024),
    )(to, mo, wr)
    return to.reshape(t.shape), mo.reshape(t.shape), wr.T


def solution(mesh):
    sizes = tuple(mesh.shape[a] for a in ("grp", "gx", "gy"))
    in_specs = (
        P("grp", "gx", "gy"), P("grp", "gx", "gy"),
        P(), P(), P(), P(), P(), P(),
        P(("grp", "gx", "gy"), None), P("gx", "gy"),
    )
    out_specs = (P("grp", "gx", "gy"), P("grp", "gx", "gy"), P(("grp", "gx", "gy"), None))
    return jax.shard_map(
        functools.partial(body, sizes), mesh=mesh, in_specs=in_specs, out_specs=out_specs, check_vma=False
    )
```

```python
import functools
import math

import jax
import jax.numpy as jnp
from jax import lax
from jax.experimental import pallas as pl
from jax.experimental.pallas import tpu as pltpu
from jax.sharding import PartitionSpec as P

SWEEPS = 8
NU_H = 0.15
NU_V = 0.15
HEATING_INTERVAL = 0.5
LEV = 32
ROWS = 16
COLS = 128
H = 8
XR = ROWS + 2 * H
UP, OWN, DOWN, ALL = 8, 16, 48, 64
G = 112
GB = 4
F32 = jnp.float32
MESH = pl.DeviceIdType.MESH
HI = lax.Precision.HIGHEST


def lanes(shape):
    return lax.broadcasted_iota(jnp.int32, shape, len(shape) - 1)


def subs(shape):
    return lax.broadcasted_iota(jnp.int32, shape, len(shape) - 2)


def roll(x, amount, axis=1):
    n = x.shape[axis]
    amount = amount % n
    return x if amount == 0 else pltpu.roll(x, amount, axis)


def kernel(
    sizes,
    cx_hbm, cy_hbm, k_hbm, d_hbm, sw_hbm, lw_hbm,
    t_hbm, m_hbm, flags_hbm, slot_hbm,
    to_ref, mo_ref, wr_ref,
    cx_ref, cy_ref, k_ref, d_ref, sw_ref, lw_ref,
    tin, min_, fin, sin,
    fs, es, coef, arad, crad, trad, acc, fsend, frecv, a0r, c0b,
    oh, fc, pws, wrecv, cus, ews, ewl, ewr,
    eos, eol, eor, els, ell, elr, hst, hland, cst, cland, lland,
    load, send, recv,
):
    ng, nx, ny = sizes
    g, x, y = lax.axis_index("grp"), lax.axis_index("gx"), lax.axis_index("gy")
    og = 1 - g
    xn, xp = lax.rem(x + 1, nx), lax.rem(x + nx - 1, nx)
    yn, yp = lax.rem(y + 1, ny), lax.rem(y + ny - 1, ny)
    gf = g.astype(F32)
    peers = [(og, x, y), (g, xn, y), (g, xp, y), (og, xn, y), (og, xp, y), (g, x, yn), (g, x, yp)]

    barrier = pltpu.get_barrier_semaphore()
    for peer in peers:
        pl.semaphore_signal(barrier, inc=1, device_id=peer, device_id_type=MESH)
    loads = [
        pltpu.make_async_copy(src, dst, load.at[n])
        for n, (src, dst) in enumerate((
            (m_hbm, min_), (t_hbm, tin), (flags_hbm, fin), (slot_hbm, sin), (cx_hbm, cx_ref),
            (cy_hbm, cy_ref), (k_hbm, k_ref), (d_hbm, d_ref), (sw_hbm, sw_ref), (lw_hbm, lw_ref),
        ))
    ]
    for c in loads:
        c.start()

    def copy(i, src, dst, peer):
        return pltpu.make_async_remote_copy(
            src_ref=src, dst_ref=dst, send_sem=send.at[i], recv_sem=recv.at[i],
            device_id=peer, device_id_type=MESH,
        )

    own = pl.ds(OWN, LEV)
    zero8 = jnp.zeros((8, COLS), F32)

    for c in loads[:2]:
        c.wait()

    def place(b, _):
        for j in range(4):
            r = 4 * b + j
            fs[0, 0, H + r, own, :] = tin[pl.ds(r, LEV, stride=ROWS), :]
            fs[0, 1, H + r, own, :] = roll(min_[pl.ds(r, LEV, stride=ROWS), :], 64)
        return 0

    lax.fori_loop(0, ROWS // 4, place, 0)
    for c in loads[2:]:
        c.wait()
    pl.semaphore_wait(barrier, len(peers))

    face = pl.ds(pl.multiple_of(DOWN - 8 - 24 * g, 8), H)
    mid = pl.ds(H, ROWS)
    levels_in = [
        copy(4, fs.at[0, :, mid, face, :], lland, (og, x, y)),
        copy(5, cst.at[0], cland.at[0], (og, xn, y)),
        copy(6, cst.at[1], cland.at[1], (og, xp, y)),
    ]
    rows_low = copy(2, hst.at[0], hland.at[0], (g, xn, y))
    rows_high = copy(3, hst.at[1], hland.at[1], (g, xp, y))

    sub = subs((H, COLS))
    for n in range(2):
        for part in range(2):
            def row(d, n=n, part=part):
                return fs[0, part, 7 + d if n else 24 - d, face, :]

            for d in range(1, 4):
                first_group = jnp.where(sub >= d, row(d), roll(row(8 - d), d, 0))
                second_group = jnp.where(sub < 8 - d, row(d), roll(row(8 - d), 8 - d, 0))
                cst[n, 4 * part + d - 1] = jnp.where(g == 0, first_group, second_group)
            cst[n, 4 * part + 3] = row(4)
    for c in levels_in[1:]:
        c.start()

    for part in range(2):
        for r in range(H):
            hst[0, H * part + r] = fs[0, part, ROWS + r, own, :]
            hst[1, H * part + r] = fs[0, part, H + r, own, :]

    lane = lanes((LEV, COLS))
    outer = (lane < 8) | (lane >= COLS - 8)
    seats = [(lane + COLS + 8 - 16 * j) % 64 < 16 for j in range(4)]
    from_left = (lane + 8) % 16 < 8

    def pack(row, at=own, n=LEV):
        total = None
        for j in range(4):
            edge = jnp.where(outer[:n], fs[0, 0, row + j, at, :], fs[0, 1, row + j, at, :])
            edge = roll(edge, 16 * j)
            total = edge if total is None else jnp.where(seats[j][:n], edge, total)
        return total

    for t in range(4):
        eos[t] = pack(H + 4 * t)
    edges_own = [copy(7, eos, eol, (g, x, yn)), copy(8, eos, eor, (g, x, yp))]
    for c in edges_own:
        c.start()

    kk = lax.broadcasted_iota(jnp.int32, (2 * COLS, COLS), 0)
    nn = lax.broadcasted_iota(jnp.int32, (2 * COLS, COLS), 1)
    means = []
    for f in range(2):
        column = (kk + COLS - 64 * f) % COLS
        pick = jnp.where(nn == (kk // COLS) * 64 + column // 2, 0.25, 0.0).astype(F32)
        parts = []
        for q in range(4):
            rows = [fs[0, f, H + 4 * q + n, own, :] for n in range(4)]
            parts.append(jnp.concatenate([rows[0] + rows[1], rows[2] + rows[3]], axis=1))
        means.append(jnp.dot(jnp.concatenate(parts, axis=0), pick, precision=HI, preferred_element_type=F32))
    heatq = 1.0 + 0.1 * means[0]
    m = means[1]
    absorber = jnp.maximum(m, 0.0) + jnp.log1p(jnp.exp(-jnp.abs(m)))
    for q in range(4):
        for seg in range(2):
            at = pl.ds(4 * seg + q, 16, stride=8)
            low = q * LEV + 16 * seg
            arad[at, :] = absorber[low:low + 16]
            trad[at, :] = heatq[low:low + 16]
    tot_a = arad[0:8, :]
    for s in range(1, 16):
        tot_a = tot_a + arad[8 * s:8 * s + 8, :]
    below = jnp.sum(fin[0:LEV, :].astype(F32), axis=0, keepdims=True)
    whole_a = tot_a + roll(tot_a, 4, 0)
    fsend[0:LEV, :] = fin[pl.ds(pl.multiple_of(LEV * og, 8), LEV), :].astype(F32)
    fsend[LEV:LEV + 8, 0:COLS] = whole_a
    fsend[LEV:LEV + 8, COLS:2 * COLS] = whole_a
    fsend[LEV:LEV + 1, COLS:2 * COLS] = below[:, 0:COLS]
    fsend[LEV + 1:LEV + 2, COLS:2 * COLS] = below[:, COLS:256]
    clouds = copy(0, fsend, frecv, (og, x, y))
    for c in [clouds, levels_in[0]]:
        c.start()

    for c in edges_own:
        c.wait_recv()
    for t in range(4):
        whole = jnp.where(from_left, eol[t], eor[t])
        hst[1 - t // 2, 2 * H + t % 2] = whole
        for j in range(4):
            es[0, H + 4 * t + j, own, :] = roll(whole, -16 * j)
    for c in (rows_low, rows_high):
        c.start()

    zero8 = jnp.zeros((8, COLS), F32)

    def clear(r, _):
        for n in range(SWEEPS):
            for part in range(2):
                for side in (UP, DOWN):
                    fs[n, part, r, side:side + H, :] = zero8
            for side in (UP, DOWN):
                es[n, r, side:side + H, :] = zero8
        return 0

    lax.fori_loop(0, XR, clear, 0)

    def coefs(i, _):
        level = i + 24 * g
        hx, hy = 0.5 * cx_ref[level], 0.5 * cy_ref[level]
        for n, value in enumerate((NU_H - hx, NU_H + hx, NU_H - hy, NU_H + hy)):
            value = value * (1.0 / NU_V)
            coef[n, pl.ds(OWN - 8 * g + i, 1), :] = jnp.full((1, COLS), value, F32)
        return 0

    lax.fori_loop(0, LEV + H, coefs, 0)


    slot = lax.broadcasted_iota(jnp.int32, (512, COLS), 0)
    for q in range(4):
        line = jnp.concatenate([sin[2 * q:2 * q + 1, :], sin[2 * q + 1:2 * q + 2, :]], axis=1)
        oh[:, q * COLS:(q + 1) * COLS] = jnp.where(slot == line, 1.0, 0.0).astype(jnp.bfloat16)

    mine = pl.multiple_of(256 * g, 256)
    theirs = pl.multiple_of(256 * og, 256)
    def advance(sweep, lo, n, row0, count):
        here, above, beneath = pl.ds(lo, n), pl.ds(lo - 1, n), pl.ds(lo + 1, n)
        lane = lanes((n, COLS))
        at_first, at_last = lane == 0, lane == COLS - 1
        mid_first, mid_last = lane == 64, lane == 63
        p = sweep - 1
        an, ap, bn, bp = (coef[c, here, :] for c in range(4))

        def update(centre, nxt, prv, cols_n, cols_p, up_, down):
            return (
                ((1.0 - 4.0 * NU_H - 2.0 * NU_V) / NU_V) * centre + an * nxt + ap * prv
                + bn * roll(cols_n, -1) + bp * roll(cols_p, 1) + up_ + down
            )

        for j in range(count):
            r = row0 + j
            c0, c1, ce = fs[p, 0, r, here, :], fs[p, 1, r, here, :], es[p, r, here, :]
            fs[sweep, 0, r, here, :] = update(
                c0, fs[p, 0, r + 1, here, :], fs[p, 0, r - 1, here, :],
                jnp.where(at_first, ce, c0), jnp.where(at_last, ce, c0),
                fs[p, 0, r, above, :], fs[p, 0, r, beneath, :],
            )
            fs[sweep, 1, r, here, :] = update(
                c1, fs[p, 1, r + 1, here, :], fs[p, 1, r - 1, here, :],
                jnp.where(mid_first, ce, c1), jnp.where(mid_last, ce, c1),
                fs[p, 1, r, above, :], fs[p, 1, r, beneath, :],
            )
            es[sweep, r, here, :] = update(
                ce, es[p, r + 1, here, :], es[p, r - 1, here, :],
                jnp.where(at_first, c0, jnp.where(mid_first, c1, ce)),
                jnp.where(at_last, c0, jnp.where(mid_last, c1, ce)),
                es[p, r, above, :], es[p, r, beneath, :],
            )

    def blocks(sweep, lo, n, row0, count, each):
        def block(b, _):
            advance(sweep, lo, n, row0 + b * each, each)
            return 0

        lax.fori_loop(0, count // each, block, 0)

    lo = pl.multiple_of(OWN - 8 * g, 8)

    def inner_rows(at, n):
        for sweep in range(1, SWEEPS):
            count = ROWS - 2 * sweep
            blocks(sweep, at, n, H + sweep, count, {14: 7, 12: 6, 10: 5, 8: 4, 6: 6, 4: 4, 2: 2}[count])

    inner_rows(OWN, LEV)

    clouds.wait_recv()
    fc[0:LEV, pl.ds(mine, 256)] = fin[pl.ds(pl.multiple_of(LEV * g, 8), LEV), :].astype(F32)
    fc[0:LEV, pl.ds(theirs, 256)] = frecv[0:LEV, :]
    fc[LEV:LEV + 8, pl.ds(mine, 256)] = jnp.broadcast_to(below * gf, (8, 256))
    count = jnp.concatenate([frecv[LEV:LEV + 1, COLS:256], frecv[LEV + 1:LEV + 2, COLS:256]], axis=1)
    fc[LEV:LEV + 8, pl.ds(theirs, 256)] = jnp.broadcast_to(count * gf, (8, 256))
    placed = jnp.dot(fc[...].astype(jnp.bfloat16), oh[...], preferred_element_type=F32)
    for q in range(4):
        part = placed[:, q * COLS:(q + 1) * COLS]
        for seg in range(2):
            crad[pl.ds(4 * seg + q, 16, stride=8), :] = part[16 * seg:16 * seg + 16]
            c0b[4 * seg + q:4 * seg + q + 1, :] = part[LEV:LEV + 1]
    tot_c = crad[0:8, :]
    for s in range(1, 16):
        tot_c = tot_c + crad[8 * s:8 * s + 8, :]
    second = subs((8, COLS)) >= 4
    init_a = jnp.where(second, roll(tot_a, 4, 0), 0.0) + gf * frecv[LEV:LEV + 8, 0:COLS]
    init_c = jnp.where(second, roll(tot_c, 4, 0), 0.0) + c0b[...]
    a0r[...] = init_a
    c0b[...] = init_c

    scale = -math.log2(math.e)
    acc[...] = jnp.zeros_like(acc)

    def radiate(block, _):
        ks, ds, ls, beams = [], [], [], []
        start_a, start_c = a0r[...], c0b[...]
        for j in range(GB):
            n = block * GB + j
            ks.append(scale * k_ref[n])
            ds.append(scale * d_ref[n])
            ls.append(lw_ref[n])
            beams.append(sw_ref[n] * jnp.exp2(start_a * ks[j] + start_c * ds[j]))
        for s in range(16):
            a, c, q = (ref[8 * s:8 * s + 8, :] for ref in (arad, crad, trad))
            total = acc[8 * s:8 * s + 8, :]
            for j in range(GB):
                e = jnp.exp2(a * ks[j] + c * ds[j])
                total = total + (beams[j] - q * ls[j]) * (1.0 - e)
                beams[j] = beams[j] * e
            acc[8 * s:8 * s + 8, :] = total
        return 0

    lax.fori_loop(0, G // GB, radiate, 0)

    tiles = []
    for q in range(4):
        both = [acc[pl.ds(4 * seg + q, 16, stride=8), :] for seg in range(2)]
        tiles.append(jnp.concatenate(both, axis=0) * (4.0 / G))
    rates = jnp.concatenate(tiles, axis=1)
    stacked = jnp.concatenate(tiles, axis=0)

    kk = lax.broadcasted_iota(jnp.int32, (COLS, 2 * COLS), 0)
    nn = lax.broadcasted_iota(jnp.int32, (COLS, 2 * COLS), 1)
    same = (kk // 64) == (nn // COLS)
    col, src = nn % COLS, kk % 64
    up = jnp.where(src == col // 2, 0.75, jnp.where(src == col // 2 - 1 + 2 * (col % 2), 0.25, 0.0))
    up = jnp.where(same, up, 0.0).astype(F32)
    refined = jnp.dot(stacked, up, precision=HI, preferred_element_type=F32)
    packed = jnp.zeros((LEV, COLS), F32)
    for i in range(8):
        q, half = i // 2, i % 2
        line = refined[q * LEV:(q + 1) * LEV, half * COLS:(half + 1) * COLS]
        cus[1 + i] = line
        here = (lane == 2 * i) | (lane == (2 * i - 1) % COLS)
        packed = jnp.where(here, roll(line, 2 * i), packed)
    ews[...] = packed
    ends = [copy(12, ews, ewl, (g, x, yn)), copy(13, ews, ewr, (g, x, yp))]
    for c in ends:
        c.start()

    rest = rates
    total = None
    for _ in range(3):
        piece = rest.astype(jnp.bfloat16)
        rest = rest - piece.astype(F32)
        part = lax.dot_general(piece, oh[...], (((1,), (1,)), ((), ())), preferred_element_type=F32)
        total = part if total is None else total + part
    pws[...] = total
    back = copy(14, pws.at[:, pl.ds(theirs, 256)], wrecv, (og, x, y))
    wr_ref[pl.ds(pl.multiple_of(LEV * g, 8), LEV), :] = pws[:, pl.ds(mine, 256)]

    for c in ends:
        c.wait_recv()
    left, right = ewl[...] * (1.0 / 3.0), ewr[...] * (1.0 / 3.0)
    for i in range(8):
        line = cus[1 + i]
        line = line + jnp.where(lane == 0, roll(left, 1 - 2 * i), 0.0)
        line = line + jnp.where(lane == COLS - 1, roll(right, COLS - 1 - 2 * i), 0.0)
        cus[1 + i] = line
    lines = [copy(15, cus.at[8], cus.at[0], (g, xn, y)), copy(16, cus.at[1], cus.at[9], (g, xp, y))]
    for c in lines:
        c.start()

    for c in levels_in:
        c.wait_recv()
    arrived = pl.ds(pl.multiple_of(DOWN - 40 * g, 8), H)

    for part in range(2):
        for r in range(ROWS):
            fs[0, part, H + r, arrived, :] = lland[part, r]
    for n in range(2):
        for part in range(2):
            def put(d, value, n=n, part=part):
                fs[0, part, 23 + d if n else 8 - d, arrived, :] = value

            for d in range(1, 4):
                both = cland[n, 4 * part + d - 1]
                put(d, both)
                put(8 - d, jnp.where(g == 1, roll(both, 8 - d, 0), roll(both, d, 0)))
            for d in (4, 8):
                put(d, cland[n, 4 * part + 3])

    def pack_levels(t, _):
        els[t] = pack(4 * t, arrived, H)
        return 0

    lax.fori_loop(0, XR // 4, pack_levels, 0)
    edges_lev = [copy(1, els, ell, (g, x, yn)), copy(11, els, elr, (g, x, yp))]
    for c in edges_lev:
        c.start()

    def take(n):
        for r in range(H):
            for part in range(2):
                fs[0, part, n * (H + ROWS) + r, own, :] = hland[n, H * part + r]
        for t in range(2):
            whole = hland[n, 2 * H + t]
            for j in range(4):
                es[0, n * (H + ROWS) + 4 * t + j, own, :] = roll(whole, -16 * j)

    def sweep_side(n):
        for sweep in range(1, SWEEPS + 1):
            advance(sweep, lo, LEV + H, XR - sweep - H if n else sweep, H)


    for c in edges_lev:
        c.wait_recv()

    def settle(t, _):
        whole = jnp.where(from_left[:H], ell[t], elr[t])
        for j in range(4):
            es[0, 4 * t + j, arrived, :] = roll(whole, -16 * j)
        return 0

    lax.fori_loop(0, XR // 4, settle, 0)

    reach = pl.multiple_of(DOWN - 8 - 32 * g, 8)
    inner_rows(reach, 2 * H)
    rows_low.wait_recv()
    back.start()
    take(0)
    sweep_side(0)
    rows_high.wait_recv()
    take(1)
    sweep_side(1)

    def finish_moisture(i, _):
        for half in range(8):
            r = 8 * i + half
            mo_ref[pl.ds(r, LEV, stride=ROWS), :] = roll(NU_V ** SWEEPS * fs[SWEEPS, 1, H + r, own, :], 64)
        return 0

    lax.fori_loop(0, ROWS // 8, finish_moisture, 0)
    for c in lines:
        c.wait_recv()

    def finish(b, _):
        for n in range(8):
            i, half = 4 * b + n // 2, n % 2
            r = 2 * i + half
            heat = 0.75 * cus[1 + i] + 0.25 * cus[i + 2 * half]
            to_ref[pl.ds(r, LEV, stride=ROWS), :] = NU_V ** SWEEPS * fs[SWEEPS, 0, H + r, own, :] + HEATING_INTERVAL * heat
        return 0

    lax.fori_loop(0, ROWS // 8, finish, 0)

    back.wait_recv()
    wr_ref[pl.ds(pl.multiple_of(LEV * og, 8), LEV), :] = wrecv[...]
    for c in [clouds, rows_low, rows_high, *levels_in, *edges_own, *edges_lev, *ends, back, *lines]:
        c.wait_send()


def write_out(*refs):
    copies = [pltpu.make_async_copy(refs[n], refs[3 + n], refs[6].at[n]) for n in range(3)]
    for c in copies:
        c.start()
    for c in copies:
        c.wait()


def body(sizes, t, m, cx, cy, k, d, sw, lw, flags, slots):
    vmem = pl.BlockSpec(memory_space=pltpu.VMEM)
    hbm = pl.BlockSpec(memory_space=pltpu.HBM)
    flat = (LEV * ROWS, COLS)
    scratch = [
        *[pltpu.SMEM((n,), F32) for n in (64, 64, G, G, G, G)],
        pltpu.VMEM(flat, F32),
        pltpu.VMEM(flat, F32),
        pltpu.VMEM((2 * LEV, 256), jnp.int32),
        pltpu.VMEM((8, 64), jnp.int32),
        pltpu.VMEM((SWEEPS + 1, 2, XR, ALL, COLS), F32),
        pltpu.VMEM((SWEEPS + 1, XR, ALL, COLS), F32),
        pltpu.VMEM((4, ALL, COLS), F32),
        pltpu.VMEM((128, COLS), F32),
        pltpu.VMEM((128, COLS), F32),
        pltpu.VMEM((128, COLS), F32),
        pltpu.VMEM((128, COLS), F32),
        pltpu.VMEM((LEV + 8, 256), F32),
        pltpu.VMEM((LEV + 8, 256), F32),
        pltpu.VMEM((8, COLS), F32),
        pltpu.VMEM((8, COLS), F32),
        pltpu.VMEM((512, 512), jnp.bfloat16),
        pltpu.VMEM((LEV + 8, 512), F32),
        pltpu.VMEM((LEV, 512), F32),
        pltpu.VMEM((LEV, 256), F32),
        pltpu.VMEM((10, LEV, COLS), F32),
        pltpu.VMEM((LEV, COLS), F32),
        pltpu.VMEM((LEV, COLS), F32),
        pltpu.VMEM((LEV, COLS), F32),
        pltpu.VMEM((4, LEV, COLS), F32),
        pltpu.VMEM((4, LEV, COLS), F32),
        pltpu.VMEM((4, LEV, COLS), F32),
        pltpu.VMEM((8, H, COLS), F32),
        pltpu.VMEM((8, H, COLS), F32),
        pltpu.VMEM((8, H, COLS), F32),
        pltpu.VMEM((2, 2 * H + 2, LEV, COLS), F32),
        pltpu.VMEM((2, 2 * H + 2, LEV, COLS), F32),
        pltpu.VMEM((2, 8, H, COLS), F32),
        pltpu.VMEM((2, 8, H, COLS), F32),
        pltpu.VMEM((2, ROWS, H, COLS), F32),
        pltpu.SemaphoreType.DMA((10,)),
        pltpu.SemaphoreType.DMA((19,)),
        pltpu.SemaphoreType.DMA((19,)),
    ]
    to, mo, wr = pl.pallas_call(
        functools.partial(kernel, sizes),
        out_shape=(pltpu.VMEM(flat, F32), pltpu.VMEM(flat, F32), pltpu.VMEM((2 * LEV, 256), F32)),
        in_specs=[hbm] * 10,
        out_specs=(vmem, vmem, vmem),
        scratch_shapes=scratch,
        compiler_params=pltpu.CompilerParams(
            collective_id=0, has_side_effects=True, vmem_limit_bytes=67043328 - 640 * 1024
        ),
    )(cx, cy, k, d, sw, lw, t.reshape(flat), m.reshape(flat), flags.T, slots)
    to, mo, wr = pl.pallas_call(
        write_out,
        out_shape=tuple(jax.ShapeDtypeStruct(v.shape, F32) for v in (to, mo, wr)),
        in_specs=[vmem] * 3,
        out_specs=(hbm,) * 3,
        scratch_shapes=[pltpu.SemaphoreType.DMA((3,))],
        compiler_params=pltpu.CompilerParams(vmem_limit_bytes=1024 * 1024),
    )(to, mo, wr)
    return to.reshape(t.shape), mo.reshape(t.shape), wr.T


def solution(mesh):
    sizes = tuple(mesh.shape[a] for a in ("grp", "gx", "gy"))
    in_specs = (
        P("grp", "gx", "gy"), P("grp", "gx", "gy"),
        P(), P(), P(), P(), P(), P(),
        P(("grp", "gx", "gy"), None), P("gx", "gy"),
    )
    out_specs = (P("grp", "gx", "gy"), P("grp", "gx", "gy"), P(("grp", "gx", "gy"), None))
    return jax.shard_map(
        functools.partial(body, sizes), mesh=mesh, in_specs=in_specs, out_specs=out_specs, check_vma=False
    )
```
